16 devices in a mesh: rep: 2 (over y, z), shard: 8 (over x, core).
Axes of the slice: x: 4, y: 2, z: 1, core: 2. Of those that a mesh axis runs over, the one named last changes fastest.
The devices are a block of a 4x4x8 slice.
Arguments:
- ratings: float32 [1024, 4096], P(('rep', 'shard')), parts along dimension 0
- observed: int32 [1024, 4096], P(('rep', 'shard')), parts along dimension 0
- user_init: float32 [1024, 128], P(('rep', 'shard')), parts along dimension 0
- item_init: float32 [8192, 128], P(('rep', 'shard')), parts along dimension 0
Outputs:
- output 1: float32 [1024, 128], P(('rep', 'shard')), parts along dimension 0
- output 2: float32 [8192, 128], P(('rep', 'shard')), parts along dimension 0
There are 2 independent parts. The reference program is written for one: setup_inputs(seed, part) draws one part's arguments, and reference() takes and returns one part's arrays. A program takes and returns all parts, laid end to end along the dimension named above; each array names one.
All inputs are finite; a program needn't handle non-finite values.
Results may differ from the reference program's by a relative error of at most 0.00254815.
Values are sent between devices in bfloat16 or wider.
A program may use at most 768 MiB of HBM per device.

```python
import jax
import jax.numpy as jnp
import math
from jax import lax

GROUP_DEVS = 8
USERS_DEV = 64
ITEMS_DEV = 512
FACTOR_RANK = 128
STRATUM_STEPS = 4
EPOCHS = 2

USERS = USERS_DEV * GROUP_DEVS
ITEMS = ITEMS_DEV * GROUP_DEVS
STEP_SCALE = (USERS_DEV + ITEMS_DEV + FACTOR_RANK) / math.sqrt(FACTOR_RANK)
STEP_SIZE = 0.5 / STEP_SCALE
WEIGHT_DECAY = 0.03 * math.sqrt(USERS_DEV * ITEMS_DEV / FACTOR_RANK)


def setup_inputs(seed: int = 0, part: int = 0) -> dict:
    base_key = jax.random.fold_in(jax.random.key(seed), part)
    sub_keys = jax.random.split(base_key, 6)
    init_scale = FACTOR_RANK ** -0.25
    true_users = jax.random.normal(sub_keys[0], (USERS, FACTOR_RANK), jnp.float32) * init_scale
    true_items = jax.random.normal(sub_keys[1], (ITEMS, FACTOR_RANK), jnp.float32) * init_scale
    rating_noise = 0.3 * jax.random.normal(sub_keys[2], (USERS, ITEMS), jnp.float32)
    ratings = jnp.dot(true_users, true_items.T) + rating_noise
    observed = (jax.random.randint(sub_keys[3], (USERS, ITEMS), 0, 10) < 3).astype(jnp.int32)
    user_init = jax.random.normal(sub_keys[4], (USERS, FACTOR_RANK), jnp.float32) * init_scale
    item_init = jax.random.normal(sub_keys[5], (ITEMS, FACTOR_RANK), jnp.float32) * init_scale
    return {"ratings": ratings, "observed": observed, "user_init": user_init, "item_init": item_init}


def to_bf16(values):
    return values.astype(jnp.bfloat16).astype(jnp.float32)


def reference(ratings, observed, user_init, item_init):
    rating_grid = ratings.reshape(GROUP_DEVS, USERS_DEV, GROUP_DEVS, ITEMS_DEV)
    seen_grid = (observed != 0).reshape(GROUP_DEVS, USERS_DEV, GROUP_DEVS, ITEMS_DEV)
    dev_ids = jnp.arange(GROUP_DEVS)
    user_blocks = user_init.reshape(GROUP_DEVS, USERS_DEV, FACTOR_RANK)
    held_items = item_init.reshape(GROUP_DEVS, ITEMS_DEV, FACTOR_RANK)

    def stratum(loop_state, stratum_idx):
        user_now, held_now = loop_state
        col_ids = (dev_ids + stratum_idx) % GROUP_DEVS
        rating_blk = rating_grid[dev_ids, :, col_ids]
        seen_blk = seen_grid[dev_ids, :, col_ids]

        def step(state_pair, unused):
            user_cur, item_cur = state_pair
            item_bf = to_bf16(item_cur)
            predicted = jnp.einsum("pur,pir->pui", to_bf16(user_cur), item_bf)
            residual = to_bf16(jnp.where(seen_blk, predicted - rating_blk, 0.0))
            user_new = user_cur - STEP_SIZE * (jnp.einsum("pui,pir->pur", residual, item_bf) + WEIGHT_DECAY * user_cur)
            user_bf = to_bf16(user_new)
            predicted = jnp.einsum("pur,pir->pui", user_bf, item_bf)
            residual = to_bf16(jnp.where(seen_blk, predicted - rating_blk, 0.0))
            item_new = item_cur - STEP_SIZE * (jnp.einsum("pui,pur->pir", residual, user_bf) + WEIGHT_DECAY * item_cur)
            return (user_new, item_new), None

        (user_now, held_now), unused = lax.scan(step, (user_now, held_now), None, length=STRATUM_STEPS)
        held_now = jnp.roll(held_now, -1, axis=0)
        return (user_now, held_now), None

    stratum_order = jnp.tile(dev_ids, EPOCHS)
    (user_blocks, held_items), unused = lax.scan(stratum, (user_blocks, held_items), stratum_order)
    return user_blocks.reshape(USERS, FACTOR_RANK), held_items.reshape(ITEMS, FACTOR_RANK)
```

```python
import functools
import math

import jax
import jax.numpy as jnp
from jax import lax
from jax.experimental import pallas as pl
from jax.experimental.pallas import tpu as pltpu
from jax.sharding import PartitionSpec as P

STRATUM_STEPS = 4
EPOCHS = 2
MESH = pl.DeviceIdType.MESH
F32 = jnp.float32
BF16 = jnp.bfloat16


def kernel(
    n, eta, lam, r_ref, m_ref, u_ref, v_ref, uo_ref, vo_ref,
    rp, rin, ubuf, vt, rsend, rrecv, usend, urecv,
):
    users, rank = u_ref.shape
    items = v_ref.shape[0]
    me = lax.axis_index("shard")
    right = lax.rem(me + 1, n)
    keep = 1.0 - eta * lam

    barrier = pltpu.get_barrier_semaphore()
    for d in range(1, n):
        pl.semaphore_signal(barrier, inc=1, device_id={"shard": lax.rem(me + d, n)}, device_id_type=MESH)

    for t in range(n):
        j = lax.rem(me + t, n)
        cols = pl.ds(pl.multiple_of(j * items, items), items)
        blk = jnp.where(m_ref[:, cols] != 0, r_ref[:, cols], jnp.inf)
        if t == 0:
            rin[0] = blk
        else:
            rp[t - 1] = blk
    vt[...] = v_ref[...].T
    ubuf[0] = u_ref[...]

    pl.semaphore_wait(barrier, n - 1)

    def r_copy(t):
        return pltpu.make_async_remote_copy(
            src_ref=rp.at[t - 1], dst_ref=rin.at[t], send_sem=rsend.at[t - 1], recv_sem=rrecv.at[t - 1],
            device_id={"shard": lax.rem(me + t, n)}, device_id_type=MESH,
        )

    def u_copy(s):
        return pltpu.make_async_remote_copy(
            src_ref=ubuf.at[s], dst_ref=ubuf.at[s + 1], send_sem=usend.at[s], recv_sem=urecv.at[s],
            device_id={"shard": right}, device_id_type=MESH,
        )

    for t in range(1, n):
        r_copy(t).start()

    def residual(ub, vb, t):
        pred = jnp.dot(ub, vb, preferred_element_type=F32)
        rat = rin[t]
        return jnp.where(rat < jnp.inf, pred - rat, 0.0).astype(BF16)

    def user_step(u, t):
        vb = vt[...].astype(BF16)
        err = residual(u.astype(BF16), vb, t)
        grad = lax.dot_general(err, vb, (((1,), (1,)), ((), ())), preferred_element_type=F32)
        return keep * u - eta * grad

    def item_step(u, t):
        v = vt[...]
        ub = u.astype(BF16)
        err = residual(ub, v.astype(BF16), t)
        grad = jnp.dot(u.T.astype(BF16), err, preferred_element_type=F32)
        vt[...] = keep * v - eta * grad

    def stratum(s, t):
        u = user_step(ubuf[s], t)

        def pair(_, u):
            item_step(u, t)
            return user_step(u, t)

        u = lax.fori_loop(0, STRATUM_STEPS - 1, pair, u)
        ubuf[s] = u
        u_copy(s).start()
        item_step(u, t)
        u_copy(s).wait()

    def first_epoch(s, carry):
        stratum(s, s)

        @pl.when(s + 1 < n)
        def _():
            r_copy(s + 1).wait()

        return carry

    def later_epoch(s, carry):
        stratum(s, lax.rem(s, n))
        return carry

    lax.fori_loop(0, n, first_epoch, 0)
    lax.fori_loop(n, EPOCHS * n, later_epoch, 0)
    uo_ref[...] = ubuf[EPOCHS * n]
    vo_ref[...] = vt[...].T


def solution(mesh):
    n = mesh.shape["shard"]
    row_spec = P(("rep", "shard"), None)

    def local(ratings, observed, user_init, item_init):
        users, rank = user_init.shape
        items = item_init.shape[0]
        scale = (users + items + rank) / math.sqrt(rank)
        eta = 0.5 / scale
        lam = 0.03 * math.sqrt(users * items / rank)
        vm = pl.BlockSpec(memory_space=pltpu.VMEM)
        steps = EPOCHS * n
        return pl.pallas_call(
            functools.partial(kernel, n, eta, lam),
            out_shape=(
                jax.ShapeDtypeStruct(user_init.shape, F32),
                jax.ShapeDtypeStruct(item_init.shape, F32),
            ),
            in_specs=[vm] * 4,
            out_specs=(vm, vm),
            scratch_shapes=[
                pltpu.VMEM((n - 1, users, items), F32),
                pltpu.VMEM((n, users, items), F32),
                pltpu.VMEM((steps + 1, users, rank), F32),
                pltpu.VMEM((rank, items), F32),
                pltpu.SemaphoreType.DMA((n - 1,)),
                pltpu.SemaphoreType.DMA((n - 1,)),
                pltpu.SemaphoreType.DMA((steps,)),
                pltpu.SemaphoreType.DMA((steps,)),
            ],
            compiler_params=pltpu.CompilerParams(collective_id=0, has_side_effects=True),
        )(ratings, observed, user_init, item_init)

    return jax.shard_map(local, mesh=mesh, in_specs=(row_spec,) * 4, out_specs=(row_spec, row_spec), check_vma=False)
```

```python
import functools
import math

import jax
import jax.numpy as jnp
from jax import lax
from jax.experimental import pallas as pl
from jax.experimental.pallas import tpu as pltpu
from jax.sharding import PartitionSpec as P

STRATUM_STEPS = 4
EPOCHS = 2
MESH = pl.DeviceIdType.MESH
F32 = jnp.float32
BF16 = jnp.bfloat16


def kernel(
    n, eta, lam, r_ref, m_ref, u_ref, v_ref, uo_ref, vo_ref,
    rbuf, mbuf, vbuf, rp, rin, ubuf, vt, rload, mload, uvload, rsend, rrecv, usend, urecv,
):
    users, rank = u_ref.shape
    items = v_ref.shape[0]
    me = lax.axis_index("shard")
    right = lax.rem(me + 1, n)
    keep = 1.0 - eta * lam

    def cols(t):
        return pl.ds(pl.multiple_of(lax.rem(me + t, n) * items, items), items)

    def r_load(t):
        return pltpu.make_async_copy(r_ref.at[:, cols(t)], rbuf.at[t], rload.at[t])

    def m_load(t):
        return pltpu.make_async_copy(m_ref.at[:, cols(t)], mbuf.at[t], mload.at[t])

    u_load = pltpu.make_async_copy(u_ref, ubuf.at[0], uvload.at[0])
    v_load = pltpu.make_async_copy(v_ref, vbuf, uvload.at[1])

    def masked(t):
        r_load(t).wait()
        m_load(t).wait()
        return jnp.where(mbuf[t] != 0, rbuf[t], jnp.inf)

    def r_copy(t):
        return pltpu.make_async_remote_copy(
            src_ref=rp.at[t - 1], dst_ref=rin.at[t], send_sem=rsend.at[t - 1], recv_sem=rrecv.at[t - 1],
            device_id={"shard": lax.rem(me + t, n)}, device_id_type=MESH,
        )

    def u_copy(s):
        return pltpu.make_async_remote_copy(
            src_ref=ubuf.at[s], dst_ref=ubuf.at[s + 1], send_sem=usend.at[s], recv_sem=urecv.at[s],
            device_id={"shard": right}, device_id_type=MESH,
        )

    v_load.start()
    u_load.start()
    for t in range(n):
        r_load(t).start()
        m_load(t).start()

    barrier = pltpu.get_barrier_semaphore()
    for d in range(1, n):
        pl.semaphore_signal(barrier, inc=1, device_id={"shard": lax.rem(me + d, n)}, device_id_type=MESH)

    v_load.wait()
    vt[...] = vbuf[...].T
    u_load.wait()
    rin[0] = masked(0)
    rp[0] = masked(1)
    pl.semaphore_wait(barrier, n - 1)
    r_copy(1).start()

    def residual(ub, vb, t):
        pred = jnp.dot(ub, vb, preferred_element_type=F32)
        rat = rin[t]
        return jnp.where(rat < jnp.inf, pred - rat, 0.0).astype(BF16)

    def user_step(u, t):
        vb = vt[...].astype(BF16)
        err = residual(u.astype(BF16), vb, t)
        grad = lax.dot_general(err, vb, (((1,), (1,)), ((), ())), preferred_element_type=F32)
        return keep * u - eta * grad

    def item_step(u, t):
        v = vt[...]
        ub = u.astype(BF16)
        err = residual(ub, v.astype(BF16), t)
        grad = jnp.dot(u.T.astype(BF16), err, preferred_element_type=F32)
        vt[...] = keep * v - eta * grad

    def stratum(s, t, after_send):
        u = user_step(ubuf[s], t)
        for _ in range(STRATUM_STEPS - 1):
            item_step(u, t)
            u = user_step(u, t)
        ubuf[s] = u
        u_copy(s).start()
        after_send()
        item_step(u, t)
        u_copy(s).wait()

    def first_epoch(s, carry):
        def send_ahead():
            @pl.when(s + 2 < n)
            def _():
                rp[s + 1] = masked(s + 2)
                r_copy(s + 2).start()

        stratum(s, s, send_ahead)

        @pl.when(s + 1 < n)
        def _():
            r_copy(s + 1).wait_recv()

        return carry

    def later_epoch(s, carry):
        stratum(s, lax.rem(s, n), lambda: None)
        return carry

    lax.fori_loop(0, n, first_epoch, 0)
    lax.fori_loop(n, EPOCHS * n, later_epoch, 0)
    for t in range(1, n):
        r_copy(t).wait_send()
    uo_ref[...] = ubuf[EPOCHS * n]
    vo_ref[...] = vt[...].T


def solution(mesh):
    n = mesh.shape["shard"]
    row_spec = P(("rep", "shard"), None)

    def local(ratings, observed, user_init, item_init):
        users, rank = user_init.shape
        items = item_init.shape[0]
        scale = (users + items + rank) / math.sqrt(rank)
        eta = 0.5 / scale
        lam = 0.03 * math.sqrt(users * items / rank)
        vmem = pl.BlockSpec(memory_space=pltpu.VMEM)
        steps = EPOCHS * n
        return pl.pallas_call(
            functools.partial(kernel, n, eta, lam),
            out_shape=(pltpu.VMEM(user_init.shape, F32), pltpu.VMEM(item_init.shape, F32)),
            in_specs=[pl.BlockSpec(memory_space=pltpu.HBM)] * 4,
            out_specs=(vmem, vmem),
            scratch_shapes=[
                pltpu.VMEM((n, users, items), F32),
                pltpu.VMEM((n, users, items), jnp.int32),
                pltpu.VMEM((items, rank), F32),
                pltpu.VMEM((n - 1, users, items), F32),
                pltpu.VMEM((n, users, items), F32),
                pltpu.VMEM((steps + 1, users, rank), F32),
                pltpu.VMEM((rank, items), F32),
                pltpu.SemaphoreType.DMA((n,)),
                pltpu.SemaphoreType.DMA((n,)),
                pltpu.SemaphoreType.DMA((2,)),
                pltpu.SemaphoreType.DMA((n - 1,)),
                pltpu.SemaphoreType.DMA((n - 1,)),
                pltpu.SemaphoreType.DMA((steps,)),
                pltpu.SemaphoreType.DMA((steps,)),
            ],
            compiler_params=pltpu.CompilerParams(collective_id=0, has_side_effects=True),
        )(ratings, observed, user_init, item_init)

    return jax.shard_map(local, mesh=mesh, in_specs=(row_spec,) * 4, out_specs=(row_spec, row_spec), check_vma=False)
```

```python
import functools
import math

import jax
import jax.numpy as jnp
from jax import lax
from jax.experimental import pallas as pl
from jax.experimental.pallas import tpu as pltpu
from jax.sharding import PartitionSpec as P

EPOCHS = 2
MESH = pl.DeviceIdType.MESH
F32 = jnp.float32
BF16 = jnp.bfloat16
A, B = 0, 1


def kernel(
    n, eta, lam, r_ref, m_ref, u_ref, v_ref, uo_ref, vo_ref,
    rbuf, mbuf, vbuf, rp, rin, uin, uout, ucur, vt, vhome,
    rload, mload, uvload, rsend, rrecv, usend, urecv, vsend, vrecv, pace,
):
    items = v_ref.shape[0]
    steps = EPOCHS * n
    me = lax.axis_index("shard")
    worker = lax.rem(me, 2) == 1
    keep = 1.0 - eta * lam

    def dev(offset):
        return {"shard": lax.rem(me + n + offset, n)}

    barrier = pltpu.get_barrier_semaphore()
    for d in range(1, n):
        pl.semaphore_signal(barrier, inc=1, device_id=dev(d), device_id_type=MESH)

    def cols(t):
        return pl.ds(pl.multiple_of(lax.rem(me + t, n) * items, items), items)

    def r_load(t):
        return pltpu.make_async_copy(r_ref.at[:, cols(t)], rbuf.at[t], rload.at[t])

    def m_load(t):
        return pltpu.make_async_copy(m_ref.at[:, cols(t)], mbuf.at[t], mload.at[t])

    u_load = pltpu.make_async_copy(u_ref, ucur, uvload.at[0])
    v_load = pltpu.make_async_copy(v_ref, vbuf, uvload.at[1])

    def load(ts):
        for t in ts:
            r_load(t).start()
            m_load(t).start()

    def masked(t):
        r_load(t).wait()
        m_load(t).wait()
        return jnp.where(mbuf[t] != 0, rbuf[t], jnp.inf)

    def remote(src, dst, send, recv, device):
        return pltpu.make_async_remote_copy(
            src_ref=src, dst_ref=dst, send_sem=send, recv_sem=recv, device_id=device, device_id_type=MESH
        )

    def r_copy(t):
        j = lax.rem(me + t, n)
        chain = lax.rem(j, 2)
        return remote(rp.at[t], rin.at[chain, t], rsend.at[t], rrecv.at[chain, t], {"shard": j - chain + 1})

    def r_arrive(chain, t):
        remote(rp.at[t], rin.at[chain, t], rsend.at[t], rrecv.at[chain, t], dev(1)).wait_recv()

    def u_copy(s, offset=2):
        return remote(uout.at[s], uin.at[s + 1], usend.at[s], urecv.at[s + 1], dev(offset))

    def u_arrive(s):
        remote(ucur, uin.at[s], usend.at[0], urecv.at[s], dev(1)).wait_recv()

    u_first = remote(ucur, uin.at[0], usend.at[0], urecv.at[0], dev(1))
    v_first = remote(vt.at[A], vt.at[A], vsend, vrecv, dev(1))
    v_last = remote(vt.at[A], vhome, vsend, vrecv, dev(-1))

    def residual(ub, vb, chain, t):
        pred = jnp.dot(ub, vb, preferred_element_type=F32)
        rat = rin[chain, t]
        return jnp.where(rat < jnp.inf, pred - rat, 0.0).astype(BF16)

    def user_step(u, chain, t):
        vb = vt[chain].astype(BF16)
        err = residual(u.astype(BF16), vb, chain, t)
        grad = lax.dot_general(err, vb, (((1,), (1,)), ((), ())), preferred_element_type=F32)
        return keep * u - eta * grad

    def item_step(u, chain, t):
        v = vt[chain]
        err = residual(u.astype(BF16), v.astype(BF16), chain, t)
        grad = jnp.dot(u.T.astype(BF16), err, preferred_element_type=F32)
        vt[chain] = keep * v - eta * grad

    def send_ahead(s):
        @pl.when(s + 2 < n - 1)
        def _():
            rp[s + 2] = masked(s + 2)
            r_copy(s + 2).start()

        @pl.when(s + 2 == n - 1)
        def _():
            rin[A, n - 1] = masked(n - 1)

        @pl.when(s + 2 < n)
        def _():
            pl.semaphore_signal(pace, inc=1, device_id=dev(-1), device_id_type=MESH)

    def begin(u, t):
        u = user_step(u, B, t)
        item_step(u, B, t)
        u = user_step(u, B, t)
        ucur[...] = u
        item_step(u, B, t)

    def stratum(s, first, last=False):
        t = s if first else lax.rem(s, n)
        u_arrive(s)
        if first:
            @pl.when(s < n - 1)
            def _():
                r_arrive(A, s)

        a = uin[s]
        b = ucur[...]
        a = user_step(a, A, t)
        b = user_step(b, B, t)
        item_step(a, A, t)
        item_step(b, B, t)
        a = user_step(a, A, t)
        b = user_step(b, B, t)
        uout[s] = b
        u_copy(s, 1 if last else 2).start()
        if first:
            send_ahead(s)
        item_step(a, A, t)
        item_step(b, B, t)
        a = user_step(a, A, t)
        item_step(a, A, t)
        a = user_step(a, A, t)
        if last:
            item_step(a, A, t)
            ucur[...] = a
            return
        if first:
            @pl.when(s < n - 1)
            def _():
                r_arrive(B, s + 1)

        t_next = lax.rem(s + 1, n)
        b = user_step(a, B, t_next)
        item_step(a, A, t)
        item_step(b, B, t_next)
        b = user_step(b, B, t_next)
        ucur[...] = b
        item_step(b, B, t_next)

    @pl.when(worker)
    def _():
        v_load.start()
        u_load.start()
        load(range(2))
        v_load.wait()
        vt[B] = vbuf[...].T
        u_load.wait()
        rin[B, 0] = masked(0)
        rp[1] = masked(1)
        load(range(2, n))
        pl.semaphore_wait(barrier, n - 1)
        r_copy(1).start()
        begin(ucur[...], 0)
        v_first.wait_recv()

        def first_epoch(s, carry):
            stratum(s, True)
            return carry

        def later_epoch(s, carry):
            stratum(s, False)
            return carry

        lax.fori_loop(0, n, first_epoch, 0)
        lax.fori_loop(n, steps - 1, later_epoch, 0)
        stratum(steps - 1, False, last=True)
        v_last.start()
        vo_ref[...] = vt[B].T
        uo_ref[...] = ucur[...]
        for t in range(1, n - 1):
            r_copy(t).wait_send()
        for s in range(steps):
            u_copy(s).wait_send()
        v_last.wait_send()

    @pl.when(jnp.logical_not(worker))
    def _():
        v_load.start()
        u_load.start()
        load(range(2))
        v_load.wait()
        vt[A] = vbuf[...].T
        u_load.wait()
        rp[0] = masked(0)
        rp[1] = masked(1)
        load(range(2, n))
        pl.semaphore_wait(barrier, n - 1)
        v_first.start()
        u_first.start()
        r_copy(0).start()
        r_copy(1).start()

        def send(t, carry):
            rp[t] = masked(t)
            pl.semaphore_wait(pace, 1)
            r_copy(t).start()
            return carry

        lax.fori_loop(2, n, send, 0)
        for t in range(n):
            r_copy(t).wait_send()
        u_first.wait_send()
        v_first.wait_send()
        u_arrive(steps)
        uo_ref[...] = uin[steps]
        v_last.wait_recv()
        vo_ref[...] = vhome[...].T


def write_out(u_ref, v_ref, uo_ref, vo_ref, sems):
    copies = [pltpu.make_async_copy(v_ref, vo_ref, sems.at[0]), pltpu.make_async_copy(u_ref, uo_ref, sems.at[1])]
    for c in copies:
        c.start()
    for c in copies:
        c.wait()


def solution(mesh):
    n = mesh.shape["shard"]
    row_spec = P(("rep", "shard"), None)

    def local(ratings, observed, user_init, item_init):
        users, rank = user_init.shape
        items = item_init.shape[0]
        scale = (users + items + rank) / math.sqrt(rank)
        eta = 0.5 / scale
        lam = 0.03 * math.sqrt(users * items / rank)
        steps = EPOCHS * n
        vmem = pl.BlockSpec(memory_space=pltpu.VMEM)
        hbm = pl.BlockSpec(memory_space=pltpu.HBM)
        dma = pltpu.SemaphoreType.DMA
        u_last, v_last = pl.pallas_call(
            functools.partial(kernel, n, eta, lam),
            out_shape=(pltpu.VMEM(user_init.shape, F32), pltpu.VMEM(item_init.shape, F32)),
            in_specs=[hbm] * 4,
            out_specs=(vmem, vmem),
            scratch_shapes=[
                pltpu.VMEM((n, users, items), F32),
                pltpu.VMEM((n, users, items), jnp.int32),
                pltpu.VMEM((items, rank), F32),
                pltpu.VMEM((n, users, items), F32),
                pltpu.VMEM((2, n, users, items), F32),
                pltpu.VMEM((steps + 1, users, rank), F32),
                pltpu.VMEM((steps, users, rank), F32),
                pltpu.VMEM((users, rank), F32),
                pltpu.VMEM((2, rank, items), F32),
                pltpu.VMEM((rank, items), F32),
                dma((n,)),
                dma((n,)),
                dma((2,)),
                dma((n,)),
                dma((2, n)),
                dma((steps,)),
                dma((steps + 1,)),
                dma,
                dma,
                pltpu.SemaphoreType.REGULAR,
            ],
            compiler_params=pltpu.CompilerParams(collective_id=0, has_side_effects=True),
        )(ratings, observed, user_init, item_init)
        return pl.pallas_call(
            write_out,
            out_shape=(jax.ShapeDtypeStruct(user_init.shape, F32), jax.ShapeDtypeStruct(item_init.shape, F32)),
            in_specs=[vmem] * 2,
            out_specs=(hbm, hbm),
            scratch_shapes=[dma((2,))],
            compiler_params=pltpu.CompilerParams(vmem_limit_bytes=2**20),
        )(u_last, v_last)

    return jax.shard_map(local, mesh=mesh, in_specs=(row_spec,) * 4, out_specs=(row_spec, row_spec), check_vma=False)
```

```python
import functools
import math

import jax
import jax.numpy as jnp
from jax import lax
from jax.experimental import pallas as pl
from jax.experimental.pallas import tpu as pltpu
from jax.sharding import PartitionSpec as P

EPOCHS = 2
MESH = pl.DeviceIdType.MESH
F32 = jnp.float32
BF16 = jnp.bfloat16
TILE = 256
A, B = 0, 1


def kernel(
    n, eta, lam, r_ref, m_ref, u_ref, v_ref, uo_ref, vo_ref,
    rbuf, mbuf, vbuf, rp, rin, uin, uout, ucur, vt, vhome,
    rload, mload, uvload, rsend, rrecv, usend, urecv, vsend, vrecv, pace,
):
    items = v_ref.shape[0]
    steps = EPOCHS * n
    me = lax.axis_index("shard")
    worker = lax.rem(me, 2) == 1
    keep = 1.0 - eta * lam

    def dev(offset):
        return {"shard": lax.rem(me + n + offset, n)}

    barrier = pltpu.get_barrier_semaphore()
    for d in range(1, n):
        pl.semaphore_signal(barrier, inc=1, device_id=dev(d), device_id_type=MESH)

    def cols(t):
        return pl.ds(pl.multiple_of(lax.rem(me + t, n) * items, items), items)

    def r_load(t):
        return pltpu.make_async_copy(r_ref.at[:, cols(t)], rbuf.at[t], rload.at[t])

    def m_load(t):
        return pltpu.make_async_copy(m_ref.at[:, cols(t)], mbuf.at[t], mload.at[t])

    u_load = pltpu.make_async_copy(u_ref, ucur, uvload.at[0])
    v_load = pltpu.make_async_copy(v_ref, vbuf, uvload.at[1])

    def load(ts):
        for t in ts:
            r_load(t).start()
            m_load(t).start()

    def masked(t):
        r_load(t).wait()
        m_load(t).wait()
        return jnp.where(mbuf[t] != 0, rbuf[t], jnp.inf)

    def remote(src, dst, send, recv, device):
        return pltpu.make_async_remote_copy(
            src_ref=src, dst_ref=dst, send_sem=send, recv_sem=recv, device_id=device, device_id_type=MESH
        )

    def r_copy(t):
        j = lax.rem(me + t, n)
        chain = lax.rem(j, 2)
        return remote(rp.at[t], rin.at[chain, t], rsend.at[t], rrecv.at[chain, t], {"shard": j - chain + 1})

    def r_arrive(chain, t):
        remote(rp.at[t], rin.at[chain, t], rsend.at[t], rrecv.at[chain, t], dev(1)).wait_recv()

    def u_copy(s, offset=2):
        return remote(uout.at[s], uin.at[s + 1], usend.at[s], urecv.at[s + 1], dev(offset))

    def u_arrive(s):
        remote(ucur, uin.at[s], usend.at[0], urecv.at[s], dev(1)).wait_recv()

    u_first = remote(ucur, uin.at[0], usend.at[0], urecv.at[0], dev(1))
    v_first = remote(vt.at[A], vt.at[A], vsend, vrecv, dev(1))
    v_last = remote(vt.at[A], vhome, vsend, vrecv, dev(-1))

    def tile(k):
        return pl.ds(k * TILE, TILE)

    class Chain:
        def __init__(self, chain, t, u):
            self.chain, self.t, self.u = chain, t, u

        def predict(self):
            ub = self.u.astype(BF16)
            self.err = []
            for k in range(items // TILE):
                pred = jnp.dot(ub, vt[self.chain, :, tile(k)].astype(BF16), preferred_element_type=F32)
                rat = rin[self.chain, self.t, :, tile(k)]
                self.err.append(jnp.where(rat < jnp.inf, pred - rat, 0.0).astype(BF16))

        def users(self):
            new = keep * self.u
            for k in range(items // TILE):
                vb = vt[self.chain, :, tile(k)].astype(BF16)
                grad = lax.dot_general(self.err[k], vb, (((1,), (1,)), ((), ())), preferred_element_type=F32)
                new = new - eta * grad
            self.u = new

        def items(self):
            ut = self.u.T.astype(BF16)
            for k in range(items // TILE):
                grad = jnp.dot(ut, self.err[k], preferred_element_type=F32)
                vt[self.chain, :, tile(k)] = keep * vt[self.chain, :, tile(k)] - eta * grad

    def advance(order, **work):
        queue = {}
        for name, (chain, kinds) in work.items():
            queue[name] = []
            for kind in kinds:
                queue[name] += [chain.predict, chain.users if kind == "u" else chain.items]
        for name in order:
            queue[name].pop(0)()
        assert not any(queue.values())

    def send_ahead(s):
        @pl.when(s + 2 < n - 1)
        def _():
            rp[s + 2] = masked(s + 2)
            r_copy(s + 2).start()

        @pl.when(s + 2 == n - 1)
        def _():
            rin[A, n - 1] = masked(n - 1)


    def begin(u, t):
        b = Chain(B, t, u)
        advance("bbbb", b=(b, "uv"))
        advance("bb", b=(b, "u"))
        ucur[...] = b.u
        advance("bb", b=(b, "v"))

    def stratum(s, first, last=False):
        t = s if first else lax.rem(s, n)
        u_arrive(s)
        if first:
            @pl.when(s < n - 1)
            def _():
                r_arrive(A, s)

        a = Chain(A, t, uin[s])
        b = Chain(B, t, ucur[...])
        advance("abababababab", a=(a, "uvu"), b=(b, "uvu"))
        uout[s] = b.u
        u_copy(s, 1 if last else 2).start()
        if first:
            send_ahead(s)
        advance("ababaaaaaa", a=(a, "vuvu"), b=(b, "v"))
        if last:
            advance("aa", a=(a, "v"))
            ucur[...] = a.u
            return
        if first:
            @pl.when(s < n - 1)
            def _():
                r_arrive(B, s + 1)

        b = Chain(B, lax.rem(s + 1, n), a.u)
        advance("bababbbb", a=(a, "v"), b=(b, "uvu"))
        ucur[...] = b.u
        advance("bb", b=(b, "v"))

    @pl.when(worker)
    def _():
        v_load.start()
        u_load.start()
        load(range(2))
        v_load.wait()
        vt[B] = vbuf[...].T
        u_load.wait()
        rin[B, 0] = masked(0)
        rp[1] = masked(1)
        load(range(2, n))
        pl.semaphore_wait(barrier, n - 1)
        r_copy(1).start()
        begin(ucur[...], 0)
        v_first.wait_recv()

        def first_epoch(s, carry):
            stratum(s, True)
            return carry

        def later_epoch(s, carry):
            stratum(s, False)
            return carry

        lax.fori_loop(0, n, first_epoch, 0)
        lax.fori_loop(n, steps - 1, later_epoch, 0)
        stratum(steps - 1, False, last=True)
        v_last.start()
        vo_ref[...] = vt[B].T
        uo_ref[...] = ucur[...]
        for t in range(1, n - 1):
            r_copy(t).wait_send()
        for s in range(steps):
            u_copy(s).wait_send()
        v_last.wait_send()

    @pl.when(jnp.logical_not(worker))
    def _():
        v_load.start()
        u_load.start()
        load(range(2))
        v_load.wait()
        vt[A] = vbuf[...].T
        u_load.wait()
        rp[0] = masked(0)
        rp[1] = masked(1)
        load(range(2, n))
        pl.semaphore_wait(barrier, n - 1)
        v_first.start()
        u_first.start()
        r_copy(0).start()
        r_copy(1).start()
        rp[2] = masked(2)
        r_copy(2).start()

        def send(t, carry):
            rp[t] = masked(t)
            r_copy(t - 1).wait_send()
            r_copy(t).start()
            return carry

        lax.fori_loop(3, n, send, 0)
        for t in (0, 1, n - 1):
            r_copy(t).wait_send()
        u_first.wait_send()
        v_first.wait_send()
        u_arrive(steps)
        uo_ref[...] = uin[steps]
        v_last.wait_recv()
        vo_ref[...] = vhome[...].T


def write_out(u_ref, v_ref, uo_ref, vo_ref, sems):
    copies = [pltpu.make_async_copy(v_ref, vo_ref, sems.at[0]), pltpu.make_async_copy(u_ref, uo_ref, sems.at[1])]
    for c in copies:
        c.start()
    for c in copies:
        c.wait()


def solution(mesh):
    n = mesh.shape["shard"]
    row_spec = P(("rep", "shard"), None)

    def local(ratings, observed, user_init, item_init):
        users, rank = user_init.shape
        items = item_init.shape[0]
        scale = (users + items + rank) / math.sqrt(rank)
        eta = 0.5 / scale
        lam = 0.03 * math.sqrt(users * items / rank)
        steps = EPOCHS * n
        vmem = pl.BlockSpec(memory_space=pltpu.VMEM)
        hbm = pl.BlockSpec(memory_space=pltpu.HBM)
        dma = pltpu.SemaphoreType.DMA
        u_last, v_last = pl.pallas_call(
            functools.partial(kernel, n, eta, lam),
            out_shape=(pltpu.VMEM(user_init.shape, F32), pltpu.VMEM(item_init.shape, F32)),
            in_specs=[hbm] * 4,
            out_specs=(vmem, vmem),
            scratch_shapes=[
                pltpu.VMEM((n, users, items), F32),
                pltpu.VMEM((n, users, items), jnp.int32),
                pltpu.VMEM((items, rank), F32),
                pltpu.VMEM((n, users, items), F32),
                pltpu.VMEM((2, n, users, items), F32),
                pltpu.VMEM((steps + 1, users, rank), F32),
                pltpu.VMEM((steps, users, rank), F32),
                pltpu.VMEM((users, rank), F32),
                pltpu.VMEM((2, rank, items), F32),
                pltpu.VMEM((rank, items), F32),
                dma((n,)),
                dma((n,)),
                dma((2,)),
                dma((n,)),
                dma((2, n)),
                dma((steps,)),
                dma((steps + 1,)),
                dma,
                dma,
                pltpu.SemaphoreType.REGULAR,
            ],
            compiler_params=pltpu.CompilerParams(collective_id=0, has_side_effects=True),
        )(ratings, observed, user_init, item_init)
        return pl.pallas_call(
            write_out,
            out_shape=(jax.ShapeDtypeStruct(user_init.shape, F32), jax.ShapeDtypeStruct(item_init.shape, F32)),
            in_specs=[vmem] * 2,
            out_specs=(hbm, hbm),
            scratch_shapes=[dma((2,))],
            compiler_params=pltpu.CompilerParams(vmem_limit_bytes=2**20),
        )(u_last, v_last)

    return jax.shard_map(local, mesh=mesh, in_specs=(row_spec,) * 4, out_specs=(row_spec, row_spec), check_vma=False)
```

```python
import functools
import math

import jax
import jax.numpy as jnp
from jax import lax
from jax.experimental import pallas as pl
from jax.experimental.pallas import tpu as pltpu
from jax.sharding import PartitionSpec as P

EPOCHS = 2
MESH = pl.DeviceIdType.MESH
F32 = jnp.float32
BF16 = jnp.bfloat16
TILE = 256
A, B = 0, 1


def kernel(
    n, eta, lam, r_ref, m_ref, u_ref, v_ref, uo_ref, vo_ref,
    rbuf, mbuf, rall, mall, vbuf, rp, rin, uin, uout, ucur, vt, vhome,
    rload, mload, allload, uvload, rsend, rrecv, usend, urecv, vsend, vrecv, pace,
):
    items = v_ref.shape[0]
    steps = EPOCHS * n
    me = lax.axis_index("shard")
    worker = lax.rem(me, 2) == 1
    keep = 1.0 - eta * lam

    def dev(offset):
        return {"shard": lax.rem(me + n + offset, n)}

    barrier = pltpu.get_barrier_semaphore()

    def greet(*offsets):
        for d in offsets:
            pl.semaphore_signal(barrier, inc=1, device_id=dev(d), device_id_type=MESH)

    def cols(t):
        return pl.ds(pl.multiple_of(lax.rem(me + t, n) * items, items), items)

    def r_load(t):
        return pltpu.make_async_copy(r_ref.at[:, cols(t)], rbuf.at[t], rload.at[t])

    def m_load(t):
        return pltpu.make_async_copy(m_ref.at[:, cols(t)], mbuf.at[t], mload.at[t])

    u_load = pltpu.make_async_copy(u_ref, ucur, uvload.at[0])
    v_load = pltpu.make_async_copy(v_ref, vbuf, uvload.at[1])

    r_all = pltpu.make_async_copy(r_ref, rall, allload.at[0])
    m_all = pltpu.make_async_copy(m_ref, mall, allload.at[1])

    def start_loads():
        v_load.start()
        u_load.start()
        for t in range(2):
            r_load(t).start()
            m_load(t).start()

    def start_rest():
        r_all.start()
        m_all.start()

    def wait_all():
        r_all.wait()
        m_all.wait()

    def masked(t):
        if isinstance(t, int) and t < 2:
            r_load(t).wait()
            m_load(t).wait()
            return jnp.where(mbuf[t] != 0, rbuf[t], jnp.inf)
        return jnp.where(mall[:, cols(t)] != 0, rall[:, cols(t)], jnp.inf)

    def remote(src, dst, send, recv, device):
        return pltpu.make_async_remote_copy(
            src_ref=src, dst_ref=dst, send_sem=send, recv_sem=recv, device_id=device, device_id_type=MESH
        )

    def r_copy(t):
        j = lax.rem(me + t, n)
        chain = lax.rem(j, 2)
        return remote(rp.at[t], rin.at[chain, t], rsend.at[t], rrecv.at[chain, t], {"shard": j - chain + 1})

    def r_arrive(chain, t):
        remote(rp.at[t], rin.at[chain, t], rsend.at[t], rrecv.at[chain, t], dev(1)).wait_recv()

    def u_copy(s, offset=2):
        return remote(uout.at[s], uin.at[s + 1], usend.at[s], urecv.at[s + 1], dev(offset))

    def u_arrive(s):
        remote(ucur, uin.at[s], usend.at[0], urecv.at[s], dev(1)).wait_recv()

    u_first = remote(ucur, uin.at[0], usend.at[0], urecv.at[0], dev(1))
    v_first = remote(vt.at[A], vt.at[A], vsend, vrecv, dev(1))
    v_last = remote(vt.at[A], vhome, vsend, vrecv, dev(-1))

    def tile(k):
        return pl.ds(k * TILE, TILE)

    class Chain:
        def __init__(self, chain, t, u):
            self.chain, self.t, self.u = chain, t, u

        def predict(self):
            ub = self.u.astype(BF16)
            self.err = []
            for k in range(items // TILE):
                pred = jnp.dot(ub, vt[self.chain, :, tile(k)].astype(BF16), preferred_element_type=F32)
                rat = rin[self.chain, self.t, :, tile(k)]
                self.err.append(jnp.where(rat < jnp.inf, pred - rat, 0.0).astype(BF16))

        def users(self):
            new = keep * self.u
            for k in range(items // TILE):
                vb = vt[self.chain, :, tile(k)].astype(BF16)
                grad = lax.dot_general(self.err[k], vb, (((1,), (1,)), ((), ())), preferred_element_type=F32)
                new = new - eta * grad
            self.u = new

        def items(self):
            ut = self.u.T.astype(BF16)
            for k in range(items // TILE):
                grad = jnp.dot(ut, self.err[k], preferred_element_type=F32)
                vt[self.chain, :, tile(k)] = keep * vt[self.chain, :, tile(k)] - eta * grad

    def advance(order, **work):
        queue = {}
        for name, (chain, kinds) in work.items():
            queue[name] = []
            for kind in kinds:
                queue[name] += [chain.predict, chain.users if kind == "u" else chain.items]
        for name in order:
            queue[name].pop(0)()
        assert not any(queue.values())

    ahead = [[2, n - 2], [3], list(range(4, n - 2))]

    def send_ahead(s):
        @pl.when(s == 0)
        def _():
            wait_all()

        for k, blocks in enumerate(ahead):
            @pl.when(s == k)
            def _():
                for t in blocks:
                    rp[t] = masked(t)
                    r_copy(t).start()

        @pl.when(s == len(ahead))
        def _():
            rin[A, n - 1] = masked(n - 1)

    def enter():
        pl.semaphore_wait(barrier, n // 2 + 1)
        r_copy(1).start()
        pl.semaphore_signal(pace, inc=1, device_id=dev(-1), device_id_type=MESH)

    def begin(u, t, enter):
        b = Chain(B, t, u)
        advance("bbbb", b=(b, "uv"))
        enter()
        advance("bb", b=(b, "u"))
        ucur[...] = b.u
        advance("bb", b=(b, "v"))

    def stratum(s, first, last=False):
        t = s if first else lax.rem(s, n)
        u_arrive(s)
        if first:
            @pl.when(s < n - 1)
            def _():
                r_arrive(A, s)

        a = Chain(A, t, uin[s])
        b = Chain(B, t, ucur[...])
        advance("abababababab", a=(a, "uvu"), b=(b, "uvu"))
        uout[s] = b.u
        u_copy(s, 1 if last else 2).start()
        if first:
            send_ahead(s)
        advance("ababaaaaaa", a=(a, "vuvu"), b=(b, "v"))
        if last:
            advance("aa", a=(a, "v"))
            ucur[...] = a.u
            return
        if first:
            @pl.when(s < n - 1)
            def _():
                r_arrive(B, s + 1)

        b = Chain(B, lax.rem(s + 1, n), a.u)
        advance("bababbbb", a=(a, "v"), b=(b, "uvu"))
        ucur[...] = b.u
        advance("bb", b=(b, "v"))

    @pl.when(worker)
    def _():
        greet(-1, *range(2, n, 2))
        start_loads()
        v_load.wait()
        vt[B] = vbuf[...].T
        u_load.wait()
        rin[B, 0] = masked(0)
        rp[1] = masked(1)
        start_rest()
        begin(ucur[...], 0, enter)
        v_first.wait_recv()

        def first_epoch(s, carry):
            stratum(s, True)
            return carry

        def later_epoch(s, carry):
            stratum(s, False)
            return carry

        lax.fori_loop(0, n, first_epoch, 0)
        lax.fori_loop(n, steps - 1, later_epoch, 0)
        stratum(steps - 1, False, last=True)
        v_last.start()
        vo_ref[...] = vt[B].T
        uo_ref[...] = ucur[...]
        for t in range(1, n - 1):
            r_copy(t).wait_send()
        for s in range(steps):
            u_copy(s).wait_send()
        v_last.wait_send()

    @pl.when(jnp.logical_not(worker))
    def _():
        greet(1, -1)
        start_loads()
        v_load.wait()
        vt[A] = vbuf[...].T
        pl.semaphore_wait(barrier, 1)
        v_first.start()
        u_load.wait()
        u_first.start()
        rp[0] = masked(0)
        r_copy(0).start()
        rp[1] = masked(1)
        r_copy(1).start()
        start_rest()
        wait_all()
        for t in range(2, n):
            rp[t] = masked(t)
        pl.semaphore_wait(pace, 1)
        r_copy(2).start()
        for t in range(3, n):
            r_copy(t - 1).wait_send()
            r_copy(t).start()
        for t in (0, 1, n - 1):
            r_copy(t).wait_send()
        u_first.wait_send()
        v_first.wait_send()
        u_arrive(steps)
        uo_ref[...] = uin[steps]
        v_last.wait_recv()
        vo_ref[...] = vhome[...].T


def write_out(u_ref, v_ref, uo_ref, vo_ref, sems):
    copies = [pltpu.make_async_copy(v_ref, vo_ref, sems.at[0]), pltpu.make_async_copy(u_ref, uo_ref, sems.at[1])]
    for c in copies:
        c.start()
    for c in copies:
        c.wait()


def solution(mesh):
    n = mesh.shape["shard"]
    row_spec = P(("rep", "shard"), None)

    def local(ratings, observed, user_init, item_init):
        users, rank = user_init.shape
        items = item_init.shape[0]
        scale = (users + items + rank) / math.sqrt(rank)
        eta = 0.5 / scale
        lam = 0.03 * math.sqrt(users * items / rank)
        steps = EPOCHS * n
        vmem = pl.BlockSpec(memory_space=pltpu.VMEM)
        hbm = pl.BlockSpec(memory_space=pltpu.HBM)
        dma = pltpu.SemaphoreType.DMA
        u_last, v_last = pl.pallas_call(
            functools.partial(kernel, n, eta, lam),
            out_shape=(pltpu.VMEM(user_init.shape, F32), pltpu.VMEM(item_init.shape, F32)),
            in_specs=[hbm] * 4,
            out_specs=(vmem, vmem),
            scratch_shapes=[
                pltpu.VMEM((2, users, items), F32),
                pltpu.VMEM((2, users, items), jnp.int32),
                pltpu.VMEM(ratings.shape, F32),
                pltpu.VMEM(observed.shape, jnp.int32),
                pltpu.VMEM((items, rank), F32),
                pltpu.VMEM((n, users, items), F32),
                pltpu.VMEM((2, n, users, items), F32),
                pltpu.VMEM((steps + 1, users, rank), F32),
                pltpu.VMEM((steps, users, rank), F32),
                pltpu.VMEM((users, rank), F32),
                pltpu.VMEM((2, rank, items), F32),
                pltpu.VMEM((rank, items), F32),
                dma((2,)),
                dma((2,)),
                dma((2,)),
                dma((2,)),
                dma((n,)),
                dma((2, n)),
                dma((steps,)),
                dma((steps + 1,)),
                dma,
                dma,
                pltpu.SemaphoreType.REGULAR,
            ],
            compiler_params=pltpu.CompilerParams(collective_id=0, has_side_effects=True),
        )(ratings, observed, user_init, item_init)
        return pl.pallas_call(
            write_out,
            out_shape=(jax.ShapeDtypeStruct(user_init.shape, F32), jax.ShapeDtypeStruct(item_init.shape, F32)),
            in_specs=[vmem] * 2,
            out_specs=(hbm, hbm),
            scratch_shapes=[dma((2,))],
            compiler_params=pltpu.CompilerParams(vmem_limit_bytes=2**20),
        )(u_last, v_last)

    return jax.shard_map(local, mesh=mesh, in_specs=(row_spec,) * 4, out_specs=(row_spec, row_spec), check_vma=False)
```

```python
import functools
import math

import jax
import jax.numpy as jnp
from jax import lax
from jax.experimental import pallas as pl
from jax.experimental.pallas import tpu as pltpu
from jax.sharding import PartitionSpec as P

EPOCHS = 2
MESH = pl.DeviceIdType.MESH
F32 = jnp.float32
BF16 = jnp.bfloat16
TILE = 256
A, B = 0, 1


def kernel(
    n, eta, lam, r_ref, m_ref, u_ref, v_ref, uo_ref, vo_ref,
    rbuf, mbuf, rall, mall, vbuf, rp, rin, uin, uout, ucur, vt, vhome,
    rload, mload, allload, uvload, rsend, rrecv, usend, urecv, vsend, vrecv, pace,
):
    items = v_ref.shape[0]
    steps = EPOCHS * n
    me = lax.axis_index("shard")
    worker = lax.rem(me, 2) == 1
    keep = 1.0 - eta * lam

    def dev(offset):
        return {"shard": lax.rem(me + n + offset, n)}

    barrier = pltpu.get_barrier_semaphore()

    def greet(*offsets):
        for d in offsets:
            pl.semaphore_signal(barrier, inc=1, device_id=dev(d), device_id_type=MESH)

    def cols(t):
        return pl.ds(pl.multiple_of(lax.rem(me + t, n) * items, items), items)

    def r_load(t):
        return pltpu.make_async_copy(r_ref.at[:, cols(t)], rbuf.at[t], rload.at[t])

    def m_load(t):
        return pltpu.make_async_copy(m_ref.at[:, cols(t)], mbuf.at[t], mload.at[t])

    u_load = pltpu.make_async_copy(u_ref, ucur, uvload.at[0])
    v_load = pltpu.make_async_copy(v_ref, vbuf, uvload.at[1])

    r_all = pltpu.make_async_copy(r_ref, rall, allload.at[0])
    m_all = pltpu.make_async_copy(m_ref, mall, allload.at[1])

    def start_loads():
        v_load.start()
        u_load.start()
        for t in range(2):
            r_load(t).start()
            m_load(t).start()

    def start_rest():
        r_all.start()
        m_all.start()

    def wait_all():
        r_all.wait()
        m_all.wait()

    def masked(t):
        if isinstance(t, int) and t < 2:
            r_load(t).wait()
            m_load(t).wait()
            return jnp.where(mbuf[t] != 0, rbuf[t], jnp.inf)
        return jnp.where(mall[:, cols(t)] != 0, rall[:, cols(t)], jnp.inf)

    def remote(src, dst, send, recv, device):
        return pltpu.make_async_remote_copy(
            src_ref=src, dst_ref=dst, send_sem=send, recv_sem=recv, device_id=device, device_id_type=MESH
        )

    def r_copy(t, slot=0):
        j = lax.rem(me + t, n)
        chain = lax.rem(j, 2)
        return remote(rp.at[t], rin.at[chain, t], rsend.at[slot], rrecv.at[chain, t], {"shard": j - chain + 1})

    def r_arrive(chain, t):
        remote(rp.at[t], rin.at[chain, t], rsend.at[0], rrecv.at[chain, t], dev(1)).wait_recv()

    def u_copy(s, offset=2):
        return remote(uout.at[s], uin.at[s + 1], usend, urecv.at[(s + 1) % n], dev(offset))

    def u_arrive(s):
        remote(ucur, uin.at[s], usend, urecv.at[s % n], dev(1)).wait_recv()

    u_first = remote(ucur, uin.at[0], usend, urecv.at[0], dev(1))
    v_first = remote(vt.at[A], vt.at[A], vsend, vrecv, dev(1))
    v_last = remote(vt.at[A], vhome, vsend, vrecv, dev(-1))

    def tile(k):
        return pl.ds(k * TILE, TILE)

    class Chain:
        def __init__(self, chain, t, u):
            self.chain, self.t, self.u = chain, t, u

        def predict(self):
            ub = self.u.astype(BF16)
            self.err = []
            for k in range(items // TILE):
                pred = jnp.dot(ub, vt[self.chain, :, tile(k)].astype(BF16), preferred_element_type=F32)
                rat = rin[self.chain, self.t, :, tile(k)]
                self.err.append(jnp.where(rat < jnp.inf, pred - rat, 0.0).astype(BF16))

        def users(self):
            new = keep * self.u
            for k in range(items // TILE):
                vb = vt[self.chain, :, tile(k)].astype(BF16)
                grad = lax.dot_general(self.err[k], vb, (((1,), (1,)), ((), ())), preferred_element_type=F32)
                new = new - eta * grad
            self.u = new

        def items(self):
            ut = self.u.T.astype(BF16)
            for k in range(items // TILE):
                grad = jnp.dot(ut, self.err[k], preferred_element_type=F32)
                vt[self.chain, :, tile(k)] = keep * vt[self.chain, :, tile(k)] - eta * grad

    def advance(order, **work):
        queue = {}
        for name, (chain, kinds) in work.items():
            queue[name] = []
            for kind in kinds:
                queue[name] += [chain.predict, chain.users if kind == "u" else chain.items]
        for name in order:
            queue[name].pop(0)()
        assert not any(queue.values())

    ahead = [[2, n - 2], [3], list(range(4, n - 2))]

    def send_ahead(s):
        @pl.when(s <= len(ahead))
        def _():
            @pl.when(s == 0)
            def _():
                wait_all()

            for k, blocks in enumerate(ahead):
                @pl.when(s == k)
                def _():
                    for t in blocks:
                        rp[t] = masked(t)
                        r_copy(t).start()

            @pl.when(s == len(ahead))
            def _():
                rin[A, n - 1] = masked(n - 1)

    def enter():
        pl.semaphore_wait(barrier, n // 2 + 1)
        r_copy(1).start()
        pl.semaphore_signal(pace, inc=1, device_id=dev(-1), device_id_type=MESH)

    def begin(u, t, enter):
        b = Chain(B, t, u)
        advance("bbbb", b=(b, "uv"))
        enter()
        advance("bb", b=(b, "u"))
        ucur[...] = b.u
        advance("bb", b=(b, "v"))

    def stratum(s, first, last=False):
        t = s if first else lax.rem(s, n)
        u_arrive(s)
        if first:
            r_arrive(A, s)

        a = Chain(A, t, uin[s])
        b = Chain(B, t, ucur[...])
        advance("abababababab", a=(a, "uvu"), b=(b, "uvu"))
        uout[s] = b.u
        u_copy(s, 1 if last else 2).start()
        if first:
            send_ahead(s)
        advance("ababaaaaaa", a=(a, "vuvu"), b=(b, "v"))
        if last:
            advance("aa", a=(a, "v"))
            ucur[...] = a.u
            return
        if first:
            r_arrive(B, s + 1)

        b = Chain(B, lax.rem(s + 1, n), a.u)
        advance("bababbbb", a=(a, "v"), b=(b, "uvu"))
        ucur[...] = b.u
        advance("bb", b=(b, "v"))

    @pl.when(worker)
    def _():
        greet(-1, *range(2, n, 2))
        start_loads()
        v_load.wait()
        vt[B] = vbuf[...].T
        u_load.wait()
        rin[B, 0] = masked(0)
        rp[1] = masked(1)
        start_rest()
        begin(ucur[...], 0, enter)
        v_first.wait_recv()

        def first_epoch(s, carry):
            stratum(s, True)
            return carry

        def later_epoch(s, carry):
            stratum(s, False)
            return carry

        lax.fori_loop(0, n - 1, first_epoch, 0)
        lax.fori_loop(n - 1, steps - 1, later_epoch, 0)
        stratum(steps - 1, False, last=True)
        v_last.start()
        vo_ref[...] = vt[B].T
        uo_ref[...] = ucur[...]
        sent = rp.at[pl.ds(1, n - 2)]
        pltpu.make_async_copy(sent, sent, rsend.at[0]).wait()
        pltpu.make_async_copy(uout, uout, usend).wait()
        v_last.wait_send()

    @pl.when(jnp.logical_not(worker))
    def _():
        greet(1, -1)
        start_loads()
        v_load.wait()
        vt[A] = vbuf[...].T
        pl.semaphore_wait(barrier, 1)
        v_first.start()
        u_load.wait()
        u_first.start()
        rp[0] = masked(0)
        r_copy(0, 1).start()
        rp[1] = masked(1)
        r_copy(1, 2).start()
        start_rest()
        wait_all()
        for t in range(2, n):
            rp[t] = masked(t)
        r_copy(0, 1).wait_send()
        pl.semaphore_wait(pace, 1)
        r_copy(2, 1).start()
        r_copy(1, 2).wait_send()
        for t in range(3, n):
            r_copy(t - 1, 1 + (t - 1) % 2).wait_send()
            r_copy(t, 1 + t % 2).start()
        r_copy(n - 1, 1 + (n - 1) % 2).wait_send()
        u_first.wait_send()
        v_first.wait_send()
        u_arrive(steps)
        uo_ref[...] = uin[steps]
        v_last.wait_recv()
        vo_ref[...] = vhome[...].T


def write_out(u_ref, v_ref, uo_ref, vo_ref, sems):
    copies = [pltpu.make_async_copy(v_ref, vo_ref, sems.at[0]), pltpu.make_async_copy(u_ref, uo_ref, sems.at[1])]
    for c in copies:
        c.start()
    for c in copies:
        c.wait()


def solution(mesh):
    n = mesh.shape["shard"]
    row_spec = P(("rep", "shard"), None)

    def local(ratings, observed, user_init, item_init):
        users, rank = user_init.shape
        items = item_init.shape[0]
        scale = (users + items + rank) / math.sqrt(rank)
        eta = 0.5 / scale
        lam = 0.03 * math.sqrt(users * items / rank)
        steps = EPOCHS * n
        vmem = pl.BlockSpec(memory_space=pltpu.VMEM)
        hbm = pl.BlockSpec(memory_space=pltpu.HBM)
        dma = pltpu.SemaphoreType.DMA
        u_last, v_last = pl.pallas_call(
            functools.partial(kernel, n, eta, lam),
            out_shape=(pltpu.VMEM(user_init.shape, F32), pltpu.VMEM(item_init.shape, F32)),
            in_specs=[hbm] * 4,
            out_specs=(vmem, vmem),
            scratch_shapes=[
                pltpu.VMEM((2, users, items), F32),
                pltpu.VMEM((2, users, items), jnp.int32),
                pltpu.VMEM(ratings.shape, F32),
                pltpu.VMEM(observed.shape, jnp.int32),
                pltpu.VMEM((items, rank), F32),
                pltpu.VMEM((n, users, items), F32),
                pltpu.VMEM((2, n, users, items), F32),
                pltpu.VMEM((steps + 1, users, rank), F32),
                pltpu.VMEM((steps, users, rank), F32),
                pltpu.VMEM((users, rank), F32),
                pltpu.VMEM((2, rank, items), F32),
                pltpu.VMEM((rank, items), F32),
                dma((2,)),
                dma((2,)),
                dma((2,)),
                dma((2,)),
                dma((3,)),
                dma((2, n)),
                dma,
                dma((n,)),
                dma,
                dma,
                pltpu.SemaphoreType.REGULAR,
            ],
            compiler_params=pltpu.CompilerParams(collective_id=0, has_side_effects=True),
        )(ratings, observed, user_init, item_init)
        return pl.pallas_call(
            write_out,
            out_shape=(jax.ShapeDtypeStruct(user_init.shape, F32), jax.ShapeDtypeStruct(item_init.shape, F32)),
            in_specs=[vmem] * 2,
            out_specs=(hbm, hbm),
            scratch_shapes=[dma((2,))],
            compiler_params=pltpu.CompilerParams(vmem_limit_bytes=2**20),
        )(u_last, v_last)

    return jax.shard_map(local, mesh=mesh, in_specs=(row_spec,) * 4, out_specs=(row_spec, row_spec), check_vma=False)
```

```python
import functools
import math

import jax
import jax.numpy as jnp
from jax import lax
from jax.experimental import pallas as pl
from jax.experimental.pallas import tpu as pltpu
from jax.sharding import PartitionSpec as P

EPOCHS = 2
MESH = pl.DeviceIdType.MESH
F32 = jnp.float32
BF16 = jnp.bfloat16
TILE = 256
A, B = 0, 1


def kernel(
    n, eta, lam, r_ref, m_ref, u_ref, v_ref, uo_ref, vo_ref,
    rbuf, mbuf, rall, mall, vbuf, rp, rin, uin, uout, ucur, vt, vhome,
    rload, mload, allload, uvload, rsend, rrecv, usend, urecv, vsend, vrecv, pace,
):
    items = v_ref.shape[0]
    steps = EPOCHS * n
    me = lax.axis_index("shard")
    worker = lax.rem(me, 2) == 1
    keep = 1.0 - eta * lam

    def dev(offset):
        return {"shard": lax.rem(me + n + offset, n)}

    barrier = pltpu.get_barrier_semaphore()

    def greet(*offsets):
        for d in offsets:
            pl.semaphore_signal(barrier, inc=1, device_id=dev(d), device_id_type=MESH)

    def cols(t):
        return pl.ds(pl.multiple_of(lax.rem(me + t, n) * items, items), items)

    def r_load(t):
        return pltpu.make_async_copy(r_ref.at[:, cols(t)], rbuf.at[t], rload.at[t])

    def m_load(t):
        return pltpu.make_async_copy(m_ref.at[:, cols(t)], mbuf.at[t], mload.at[t])

    u_load = pltpu.make_async_copy(u_ref, ucur, uvload.at[0])
    v_load = pltpu.make_async_copy(v_ref, vbuf, uvload.at[1])

    r_all = pltpu.make_async_copy(r_ref, rall, allload.at[0])
    m_all = pltpu.make_async_copy(m_ref, mall, allload.at[1])

    def start_loads():
        v_load.start()
        u_load.start()
        for t in range(2):
            r_load(t).start()
            m_load(t).start()

    def start_rest():
        r_all.start()
        m_all.start()

    def wait_all():
        r_all.wait()
        m_all.wait()

    def masked(t):
        if isinstance(t, int) and t < 2:
            r_load(t).wait()
            m_load(t).wait()
            return jnp.where(mbuf[t] != 0, rbuf[t], jnp.inf)
        return jnp.where(mall[:, cols(t)] != 0, rall[:, cols(t)], jnp.inf)

    def remote(src, dst, send, recv, device):
        return pltpu.make_async_remote_copy(
            src_ref=src, dst_ref=dst, send_sem=send, recv_sem=recv, device_id=device, device_id_type=MESH
        )

    def r_copy(t, slot=0):
        j = lax.rem(me + t, n)
        chain = lax.rem(j, 2)
        return remote(rp.at[t], rin.at[chain, t], rsend.at[slot], rrecv.at[chain, t], {"shard": j - chain + 1})

    def r_arrive(chain, t):
        remote(rp.at[t], rin.at[chain, t], rsend.at[0], rrecv.at[chain, t], dev(1)).wait_recv()

    def u_copy(s, offset=2):
        return remote(uout.at[s], uin.at[s + 1], usend, urecv.at[lax.rem(s + 1, n)], dev(offset))

    def u_arrive(s):
        remote(ucur, uin.at[s], usend, urecv.at[lax.rem(s, n)], dev(1)).wait_recv()

    u_first = remote(ucur, uin.at[0], usend, urecv.at[0], dev(1))
    v_first = remote(vt.at[A], vt.at[A], vsend, vrecv, dev(1))
    v_last = remote(vt.at[A], vhome, vsend, vrecv, dev(-1))

    def tile(k):
        return pl.ds(k * TILE, TILE)

    class Chain:
        def __init__(self, chain, t, u):
            self.chain, self.t, self.u = chain, t, u

        def predict(self):
            ub = self.u.astype(BF16)
            self.err = []
            for k in range(items // TILE):
                pred = jnp.dot(ub, vt[self.chain, :, tile(k)].astype(BF16), preferred_element_type=F32)
                rat = rin[self.chain, self.t, :, tile(k)]
                self.err.append(jnp.where(rat < jnp.inf, pred - rat, 0.0).astype(BF16))

        def users(self):
            new = keep * self.u
            for k in range(items // TILE):
                vb = vt[self.chain, :, tile(k)].astype(BF16)
                grad = lax.dot_general(self.err[k], vb, (((1,), (1,)), ((), ())), preferred_element_type=F32)
                new = new - eta * grad
            self.u = new

        def items(self):
            ut = self.u.T.astype(BF16)
            for k in range(items // TILE):
                grad = jnp.dot(ut, self.err[k], preferred_element_type=F32)
                vt[self.chain, :, tile(k)] = keep * vt[self.chain, :, tile(k)] - eta * grad

    def advance(order, **work):
        queue = {}
        for name, (chain, kinds) in work.items():
            queue[name] = []
            for kind in kinds:
                queue[name] += [chain.predict, chain.users if kind == "u" else chain.items]
        for name in order:
            queue[name].pop(0)()
        assert not any(queue.values())

    ahead = [[2, n - 2], [3], list(range(4, n - 2))]

    def send_ahead(s):
        @pl.when(s <= len(ahead))
        def _():
            @pl.when(s == 0)
            def _():
                wait_all()

            for k, blocks in enumerate(ahead):
                @pl.when(s == k)
                def _():
                    for t in blocks:
                        rp[t] = masked(t)
                        r_copy(t).start()

            @pl.when(s == len(ahead))
            def _():
                rin[A, n - 1] = masked(n - 1)

    def enter():
        pl.semaphore_wait(barrier, n // 2 + 1)
        r_copy(1).start()
        pl.semaphore_signal(pace, inc=1, device_id=dev(-1), device_id_type=MESH)

    def begin(u, t, enter):
        b = Chain(B, t, u)
        advance("bbbb", b=(b, "uv"))
        enter()
        advance("bb", b=(b, "u"))
        ucur[...] = b.u
        advance("bb", b=(b, "v"))

    def stratum(s, first, last=False):
        t = s if first else lax.rem(s, n)
        u_arrive(s)
        if first:
            r_arrive(A, s)

        a = Chain(A, t, uin[s])
        b = Chain(B, t, ucur[...])
        advance("abababababab", a=(a, "uvu"), b=(b, "uvu"))
        uout[s] = b.u
        u_copy(s, 1 if last else 2).start()
        if first:
            send_ahead(s)
        advance("aaababaaaa", a=(a, "vuvu"), b=(b, "v"))
        if last:
            advance("aa", a=(a, "v"))
            ucur[...] = a.u
            return
        if first:
            r_arrive(B, s + 1)

        b = Chain(B, lax.rem(s + 1, n), a.u)
        advance("bababbbb", a=(a, "v"), b=(b, "uvu"))
        ucur[...] = b.u
        advance("bb", b=(b, "v"))

    @pl.when(worker)
    def _():
        greet(-1, *range(2, n, 2))
        start_loads()
        v_load.wait()
        vt[B] = vbuf[...].T
        u_load.wait()
        rin[B, 0] = masked(0)
        rp[1] = masked(1)
        start_rest()
        begin(ucur[...], 0, enter)
        v_first.wait_recv()

        def first_epoch(s, carry):
            stratum(s, True)
            return carry

        def later_epoch(s, carry):
            stratum(s, False)
            return carry

        lax.fori_loop(0, n - 1, first_epoch, 0)
        lax.fori_loop(n - 1, steps - 1, later_epoch, 0)
        stratum(steps - 1, False, last=True)
        v_last.start()
        vo_ref[...] = vt[B].T
        uo_ref[...] = ucur[...]
        sent = rp.at[pl.ds(1, n - 2)]
        pltpu.make_async_copy(sent, sent, rsend.at[0]).wait()
        pltpu.make_async_copy(uout, uout, usend).wait()
        v_last.wait_send()

    @pl.when(jnp.logical_not(worker))
    def _():
        greet(1, -1)
        start_loads()
        v_load.wait()
        vt[A] = vbuf[...].T
        pl.semaphore_wait(barrier, 1)
        v_first.start()
        u_load.wait()
        u_first.start()
        rp[0] = masked(0)
        r_copy(0, 1).start()
        rp[1] = masked(1)
        r_copy(1, 2).start()
        start_rest()
        wait_all()
        for t in range(2, n):
            rp[t] = masked(t)
        r_copy(0, 1).wait_send()
        pl.semaphore_wait(pace, 1)
        r_copy(2, 1).start()
        r_copy(1, 2).wait_send()
        for t in range(3, n):
            r_copy(t - 1, 1 + (t - 1) % 2).wait_send()
            r_copy(t, 1 + t % 2).start()
        r_copy(n - 1, 1 + (n - 1) % 2).wait_send()
        u_first.wait_send()
        v_first.wait_send()
        u_arrive(steps)
        uo_ref[...] = uin[steps]
        v_last.wait_recv()
        vo_ref[...] = vhome[...].T


def write_out(u_ref, v_ref, uo_ref, vo_ref, sems):
    copies = [pltpu.make_async_copy(v_ref, vo_ref, sems.at[0]), pltpu.make_async_copy(u_ref, uo_ref, sems.at[1])]
    for c in copies:
        c.start()
    for c in copies:
        c.wait()


def solution(mesh):
    n = mesh.shape["shard"]
    row_spec = P(("rep", "shard"), None)

    def local(ratings, observed, user_init, item_init):
        users, rank = user_init.shape
        items = item_init.shape[0]
        scale = (users + items + rank) / math.sqrt(rank)
        eta = 0.5 / scale
        lam = 0.03 * math.sqrt(users * items / rank)
        steps = EPOCHS * n
        vmem = pl.BlockSpec(memory_space=pltpu.VMEM)
        hbm = pl.BlockSpec(memory_space=pltpu.HBM)
        dma = pltpu.SemaphoreType.DMA
        u_last, v_last = pl.pallas_call(
            functools.partial(kernel, n, eta, lam),
            out_shape=(pltpu.VMEM(user_init.shape, F32), pltpu.VMEM(item_init.shape, F32)),
            in_specs=[hbm] * 4,
            out_specs=(vmem, vmem),
            scratch_shapes=[
                pltpu.VMEM((2, users, items), F32),
                pltpu.VMEM((2, users, items), jnp.int32),
                pltpu.VMEM(ratings.shape, F32),
                pltpu.VMEM(observed.shape, jnp.int32),
                pltpu.VMEM((items, rank), F32),
                pltpu.VMEM((n, users, items), F32),
                pltpu.VMEM((2, n, users, items), F32),
                pltpu.VMEM((steps + 1, users, rank), F32),
                pltpu.VMEM((steps, users, rank), F32),
                pltpu.VMEM((users, rank), F32),
                pltpu.VMEM((2, rank, items), F32),
                pltpu.VMEM((rank, items), F32),
                dma((2,)),
                dma((2,)),
                dma((2,)),
                dma((2,)),
                dma((3,)),
                dma((2, n)),
                dma,
                dma((n,)),
                dma,
                dma,
                pltpu.SemaphoreType.REGULAR,
            ],
            compiler_params=pltpu.CompilerParams(collective_id=0, has_side_effects=True),
        )(ratings, observed, user_init, item_init)
        return pl.pallas_call(
            write_out,
            out_shape=(jax.ShapeDtypeStruct(user_init.shape, F32), jax.ShapeDtypeStruct(item_init.shape, F32)),
            in_specs=[vmem] * 2,
            out_specs=(hbm, hbm),
            scratch_shapes=[dma((2,))],
            compiler_params=pltpu.CompilerParams(vmem_limit_bytes=2**20),
        )(u_last, v_last)

    return jax.shard_map(local, mesh=mesh, in_specs=(row_spec,) * 4, out_specs=(row_spec, row_spec), check_vma=False)
```

```python
import functools
import math

import jax
import jax.numpy as jnp
from jax import lax
from jax.experimental import pallas as pl
from jax.experimental.pallas import tpu as pltpu
from jax.sharding import PartitionSpec as P

EPOCHS = 2
MESH = pl.DeviceIdType.MESH
F32 = jnp.float32
BF16 = jnp.bfloat16
TILE = 256
A, B = 0, 1


def kernel(
    n, eta, lam, r_ref, m_ref, u_ref, v_ref, uo_ref, vo_ref,
    rbuf, mbuf, rall, mall, vbuf, rp, rin, uin, uout, ucur, vt, vhome,
    rload, mload, allload, uvload, rsend, rrecv, usend, urecv, vsend, vrecv, pace,
):
    items = v_ref.shape[0]
    steps = EPOCHS * n
    me = lax.axis_index("shard")
    worker = lax.rem(me, 2) == 1
    keep = 1.0 - eta * lam

    def dev(offset):
        return {"shard": lax.rem(me + n + offset, n)}

    barrier = pltpu.get_barrier_semaphore()

    def greet(*offsets):
        for d in offsets:
            pl.semaphore_signal(barrier, inc=1, device_id=dev(d), device_id_type=MESH)

    def cols(t):
        return pl.ds(pl.multiple_of(lax.rem(me + t, n) * items, items), items)

    def r_load(t):
        return pltpu.make_async_copy(r_ref.at[:, cols(t)], rbuf.at[t], rload.at[t])

    def m_load(t):
        return pltpu.make_async_copy(m_ref.at[:, cols(t)], mbuf.at[t], mload.at[t])

    u_load = pltpu.make_async_copy(u_ref, ucur, uvload.at[0])
    v_load = pltpu.make_async_copy(v_ref, vbuf, uvload.at[1])

    r_all = pltpu.make_async_copy(r_ref, rall, allload.at[0])
    m_all = pltpu.make_async_copy(m_ref, mall, allload.at[1])

    def start_loads():
        v_load.start()
        u_load.start()
        for t in range(2):
            r_load(t).start()
            m_load(t).start()

    def start_rest():
        r_all.start()
        m_all.start()

    def wait_all():
        r_all.wait()
        m_all.wait()

    def masked(t):
        if isinstance(t, int) and t < 2:
            r_load(t).wait()
            m_load(t).wait()
            return jnp.where(mbuf[t] != 0, rbuf[t], jnp.inf)
        return jnp.where(mall[:, cols(t)] != 0, rall[:, cols(t)], jnp.inf)

    def remote(src, dst, send, recv, device):
        return pltpu.make_async_remote_copy(
            src_ref=src, dst_ref=dst, send_sem=send, recv_sem=recv, device_id=device, device_id_type=MESH
        )

    def r_copy(t, slot=0):
        j = lax.rem(me + t, n)
        chain = lax.rem(j, 2)
        return remote(rp.at[t], rin.at[chain, t], rsend.at[slot], rrecv.at[chain, t], {"shard": j - chain + 1})

    def r_arrive(chain, t):
        remote(rp.at[t], rin.at[chain, t], rsend.at[0], rrecv.at[chain, t], dev(1)).wait_recv()

    def u_copy(s, offset=2):
        return remote(uout.at[s], uin.at[s + 1], usend, urecv.at[lax.rem(s + 1, n)], dev(offset))

    def u_arrive(s):
        remote(ucur, uin.at[s], usend, urecv.at[lax.rem(s, n)], dev(1)).wait_recv()

    u_first = remote(ucur, uin.at[0], usend, urecv.at[0], dev(1))
    v_first = remote(vt.at[A], vt.at[A], vsend, vrecv, dev(1))
    v_last = remote(vt.at[A], vhome, vsend, vrecv, dev(-1))

    def tile(k):
        return pl.ds(k * TILE, TILE)

    class Chain:
        def __init__(self, chain, t, u):
            self.chain, self.t, self.u = chain, t, u

        def predict(self):
            ub = self.u.astype(BF16)
            pred = jnp.dot(ub, vt[self.chain].astype(BF16), preferred_element_type=F32)
            rat = rin[self.chain, self.t]
            err = jnp.where(rat < jnp.inf, pred - rat, 0.0).astype(BF16)
            self.err = [err[:, k * TILE:(k + 1) * TILE] for k in range(items // TILE)]

        def users(self):
            new = keep * self.u
            for k in range(items // TILE):
                vb = vt[self.chain, :, tile(k)].astype(BF16)
                grad = lax.dot_general(self.err[k], vb, (((1,), (1,)), ((), ())), preferred_element_type=F32)
                new = new - eta * grad
            self.u = new

        def items(self):
            ut = self.u.T.astype(BF16)
            for k in range(items // TILE):
                grad = jnp.dot(ut, self.err[k], preferred_element_type=F32)
                vt[self.chain, :, tile(k)] = keep * vt[self.chain, :, tile(k)] - eta * grad

    def advance(order, **work):
        queue = {}
        for name, (chain, kinds) in work.items():
            queue[name] = []
            for kind in kinds:
                queue[name] += [chain.predict, chain.users if kind == "u" else chain.items]
        for name in order:
            queue[name].pop(0)()
        assert not any(queue.values())

    ahead = [[2, n - 2], [3], list(range(4, n - 2))]

    def send_ahead(s):
        @pl.when(s <= len(ahead))
        def _():
            @pl.when(s == 0)
            def _():
                wait_all()

            for k, blocks in enumerate(ahead):
                @pl.when(s == k)
                def _():
                    for t in blocks:
                        rp[t] = masked(t)
                        r_copy(t).start()

            @pl.when(s == len(ahead))
            def _():
                rin[A, n - 1] = masked(n - 1)

    def enter():
        rp[1] = masked(1)
        pl.semaphore_wait(barrier, n // 2 + 1)
        r_copy(1).start()
        pl.semaphore_signal(pace, inc=1, device_id=dev(-1), device_id_type=MESH)

    def begin(u, t, enter):
        b = Chain(B, t, u)
        advance("bbbb", b=(b, "uv"))
        enter()
        advance("bb", b=(b, "u"))
        ucur[...] = b.u
        advance("bb", b=(b, "v"))

    def stratum(s, first, last=False):
        t = s if first else lax.rem(s, n)
        u_arrive(s)
        if first:
            r_arrive(A, s)

        a = Chain(A, t, uin[s])
        b = Chain(B, t, ucur[...])
        advance("abababababab", a=(a, "uvu"), b=(b, "uvu"))
        uout[s] = b.u
        u_copy(s, 1 if last else 2).start()
        if first:
            send_ahead(s)
        advance("aaababaaaa", a=(a, "vuvu"), b=(b, "v"))
        if last:
            advance("aa", a=(a, "v"))
            ucur[...] = a.u
            return
        if first:
            r_arrive(B, s + 1)

        b = Chain(B, lax.rem(s + 1, n), a.u)
        advance("bababbbb", a=(a, "v"), b=(b, "uvu"))
        ucur[...] = b.u
        advance("bb", b=(b, "v"))

    @pl.when(worker)
    def _():
        greet(-1, *range(2, n, 2))
        start_loads()
        v_load.wait()
        vt[B] = vbuf[...].T
        u_load.wait()
        rin[B, 0] = masked(0)
        start_rest()
        begin(ucur[...], 0, enter)
        v_first.wait_recv()

        def first_epoch(s, carry):
            stratum(s, True)
            return carry

        def later_epoch(s, carry):
            stratum(s, False)
            return carry

        lax.fori_loop(0, n - 1, first_epoch, 0)
        lax.fori_loop(n - 1, steps - 1, later_epoch, 0)
        stratum(steps - 1, False, last=True)
        v_last.start()
        vo_ref[...] = vt[B].T
        uo_ref[...] = ucur[...]
        sent = rp.at[pl.ds(1, n - 2)]
        pltpu.make_async_copy(sent, sent, rsend.at[0]).wait()
        pltpu.make_async_copy(uout, uout, usend).wait()
        v_last.wait_send()

    @pl.when(jnp.logical_not(worker))
    def _():
        greet(1, -1)
        start_loads()
        v_load.wait()
        vt[A] = vbuf[...].T
        pl.semaphore_wait(barrier, 1)
        v_first.start()
        u_load.wait()
        u_first.start()
        rp[0] = masked(0)
        r_copy(0, 1).start()
        rp[1] = masked(1)
        r_copy(1, 2).start()
        start_rest()
        wait_all()
        for t in range(2, n):
            rp[t] = masked(t)
        r_copy(0, 1).wait_send()
        pl.semaphore_wait(pace, 1)
        r_copy(2, 1).start()
        r_copy(1, 2).wait_send()
        for t in range(3, n):
            r_copy(t - 1, 1 + (t - 1) % 2).wait_send()
            r_copy(t, 1 + t % 2).start()
        r_copy(n - 1, 1 + (n - 1) % 2).wait_send()
        u_first.wait_send()
        v_first.wait_send()
        u_arrive(steps)
        uo_ref[...] = uin[steps]
        v_last.wait_recv()
        vo_ref[...] = vhome[...].T


def write_out(u_ref, v_ref, uo_ref, vo_ref, sems):
    copies = [pltpu.make_async_copy(v_ref, vo_ref, sems.at[0]), pltpu.make_async_copy(u_ref, uo_ref, sems.at[1])]
    for c in copies:
        c.start()
    for c in copies:
        c.wait()


def solution(mesh):
    n = mesh.shape["shard"]
    row_spec = P(("rep", "shard"), None)

    def local(ratings, observed, user_init, item_init):
        users, rank = user_init.shape
        items = item_init.shape[0]
        scale = (users + items + rank) / math.sqrt(rank)
        eta = 0.5 / scale
        lam = 0.03 * math.sqrt(users * items / rank)
        steps = EPOCHS * n
        vmem = pl.BlockSpec(memory_space=pltpu.VMEM)
        hbm = pl.BlockSpec(memory_space=pltpu.HBM)
        dma = pltpu.SemaphoreType.DMA
        u_last, v_last = pl.pallas_call(
            functools.partial(kernel, n, eta, lam),
            out_shape=(pltpu.VMEM(user_init.shape, F32), pltpu.VMEM(item_init.shape, F32)),
            in_specs=[hbm] * 4,
            out_specs=(vmem, vmem),
            scratch_shapes=[
                pltpu.VMEM((2, users, items), F32),
                pltpu.VMEM((2, users, items), jnp.int32),
                pltpu.VMEM(ratings.shape, F32),
                pltpu.VMEM(observed.shape, jnp.int32),
                pltpu.VMEM((items, rank), F32),
                pltpu.VMEM((n, users, items), F32),
                pltpu.VMEM((2, n, users, items), F32),
                pltpu.VMEM((steps + 1, users, rank), F32),
                pltpu.VMEM((steps, users, rank), F32),
                pltpu.VMEM((users, rank), F32),
                pltpu.VMEM((2, rank, items), F32),
                pltpu.VMEM((rank, items), F32),
                dma((2,)),
                dma((2,)),
                dma((2,)),
                dma((2,)),
                dma((3,)),
                dma((2, n)),
                dma,
                dma((n,)),
                dma,
                dma,
                pltpu.SemaphoreType.REGULAR,
            ],
            compiler_params=pltpu.CompilerParams(collective_id=0, has_side_effects=True),
        )(ratings, observed, user_init, item_init)
        return pl.pallas_call(
            write_out,
            out_shape=(jax.ShapeDtypeStruct(user_init.shape, F32), jax.ShapeDtypeStruct(item_init.shape, F32)),
            in_specs=[vmem] * 2,
            out_specs=(hbm, hbm),
            scratch_shapes=[dma((2,))],
            compiler_params=pltpu.CompilerParams(vmem_limit_bytes=2**20),
        )(u_last, v_last)

    return jax.shard_map(local, mesh=mesh, in_specs=(row_spec,) * 4, out_specs=(row_spec, row_spec), check_vma=False)
```

```python
import functools
import math

import jax
import jax.numpy as jnp
from jax import lax
from jax.experimental import pallas as pl
from jax.experimental.pallas import tpu as pltpu
from jax.sharding import PartitionSpec as P

EPOCHS = 2
MESH = pl.DeviceIdType.MESH
F32 = jnp.float32
BF16 = jnp.bfloat16
TILE = 256
A, B = 0, 1


def kernel(
    n, eta, lam, r_ref, m_ref, u_ref, v_ref, uo_ref, vo_ref,
    rbuf, mbuf, rall, mall, vbuf, rp, rin, uin, uout, ucur, vt, vhome,
    rload, allload, uvload, rsend, rrecv, usend, urecv, vsend, vrecv, pace,
):
    items = v_ref.shape[0]
    steps = EPOCHS * n
    me = lax.axis_index("shard")
    worker = lax.rem(me, 2) == 1
    keep = 1.0 - eta * lam

    def dev(offset):
        return {"shard": lax.rem(me + n + offset, n)}

    barrier = pltpu.get_barrier_semaphore()

    def greet(*offsets):
        for d in offsets:
            pl.semaphore_signal(barrier, inc=1, device_id=dev(d), device_id_type=MESH)

    def cols(t):
        return pl.ds(pl.multiple_of(lax.rem(me + t, n) * items, items), items)

    def r_load(t):
        return pltpu.make_async_copy(r_ref.at[:, cols(t)], rbuf.at[t], rload.at[t])

    def m_load(t):
        return pltpu.make_async_copy(m_ref.at[:, cols(t)], mbuf.at[t], rload.at[t])

    u_load = pltpu.make_async_copy(u_ref, ucur, uvload.at[0])
    v_load = pltpu.make_async_copy(v_ref, vbuf, uvload.at[1])

    r_all = pltpu.make_async_copy(r_ref, rall, allload)
    m_all = pltpu.make_async_copy(m_ref, mall, allload)

    def start_loads():
        v_load.start()
        u_load.start()
        for t in range(2):
            r_load(t).start()
            m_load(t).start()

    def start_rest():
        r_all.start()
        m_all.start()

    def wait_all():
        pltpu.make_async_copy(rin, rin, allload).wait()

    def masked(t):
        if isinstance(t, int) and t < 2:
            pair = rin.at[0, pl.ds(0, 2)]
            pltpu.make_async_copy(pair, pair, rload.at[t]).wait()
            return jnp.where(mbuf[t] != 0, rbuf[t], jnp.inf)
        return jnp.where(mall[:, cols(t)] != 0, rall[:, cols(t)], jnp.inf)

    def remote(src, dst, send, recv, device):
        return pltpu.make_async_remote_copy(
            src_ref=src, dst_ref=dst, send_sem=send, recv_sem=recv, device_id=device, device_id_type=MESH
        )

    def r_copy(t, slot=0):
        j = lax.rem(me + t, n)
        chain = lax.rem(j, 2)
        return remote(rp.at[t], rin.at[chain, t], rsend.at[slot], rrecv.at[chain, t], {"shard": j - chain + 1})

    def r_arrive(chain, t):
        remote(rp.at[t], rin.at[chain, t], rsend.at[0], rrecv.at[chain, t], dev(1)).wait_recv()

    def u_copy(s, offset=2):
        return remote(uout.at[s], uin.at[s + 1], usend, urecv.at[lax.rem(s + 1, n)], dev(offset))

    def u_arrive(s):
        remote(ucur, uin.at[s], usend, urecv.at[lax.rem(s, n)], dev(1)).wait_recv()

    u_first = remote(ucur, uin.at[0], usend, urecv.at[0], dev(1))
    v_first = remote(vt.at[A], vt.at[A], vsend, vrecv, dev(1))
    v_last = remote(vt.at[A], vhome, vsend, vrecv, dev(-1))

    def tile(k):
        return pl.ds(k * TILE, TILE)

    class Chain:
        def __init__(self, chain, t, u):
            self.chain, self.t, self.u = chain, t, u

        def predict(self):
            ub = self.u.astype(BF16)
            pred = jnp.dot(ub, vt[self.chain].astype(BF16), preferred_element_type=F32)
            rat = rin[self.chain, self.t]
            err = jnp.where(rat < jnp.inf, pred - rat, 0.0).astype(BF16)
            self.err = [err[:, k * TILE:(k + 1) * TILE] for k in range(items // TILE)]

        def users(self):
            new = keep * self.u
            for k in range(items // TILE):
                vb = vt[self.chain, :, tile(k)].astype(BF16)
                grad = lax.dot_general(self.err[k], vb, (((1,), (1,)), ((), ())), preferred_element_type=F32)
                new = new - eta * grad
            self.u = new

        def items(self):
            ut = self.u.T.astype(BF16)
            for k in range(items // TILE):
                grad = jnp.dot(ut, self.err[k], preferred_element_type=F32)
                vt[self.chain, :, tile(k)] = keep * vt[self.chain, :, tile(k)] - eta * grad

    def advance(order, **work):
        queue = {}
        for name, (chain, kinds) in work.items():
            queue[name] = []
            for kind in kinds:
                queue[name] += [chain.predict, chain.users if kind == "u" else chain.items]
        for name in order:
            queue[name].pop(0)()
        assert not any(queue.values())

    ahead = [[2, n - 2], [3], list(range(4, n - 2))]

    def send_ahead(s):
        @pl.when(s <= len(ahead))
        def _():
            @pl.when(s == 0)
            def _():
                wait_all()

            for k, blocks in enumerate(ahead):
                @pl.when(s == k)
                def _():
                    for t in blocks:
                        rp[t] = masked(t)
                        r_copy(t).start()

            @pl.when(s == len(ahead))
            def _():
                rin[A, n - 1] = masked(n - 1)

    def enter():
        rp[1] = masked(1)
        pl.semaphore_wait(barrier, n // 2 + 1)
        r_copy(1).start()
        pl.semaphore_signal(pace, inc=1, device_id=dev(-1), device_id_type=MESH)

    def begin(u, t, enter):
        b = Chain(B, t, u)
        advance("bbbb", b=(b, "uv"))
        enter()
        advance("bb", b=(b, "u"))
        ucur[...] = b.u
        advance("bb", b=(b, "v"))

    def stratum(s, first, last=False):
        t = s if first else lax.rem(s, n)
        u_arrive(s)
        if first:
            r_arrive(A, s)

        a = Chain(A, t, uin[s])
        b = Chain(B, t, ucur[...])
        advance("abababababab", a=(a, "uvu"), b=(b, "uvu"))
        uout[s] = b.u
        u_copy(s, 1 if last else 2).start()
        if first:
            send_ahead(s)
        advance("aaababaaaa", a=(a, "vuvu"), b=(b, "v"))
        if last:
            advance("aa", a=(a, "v"))
            ucur[...] = a.u
            return
        if first:
            r_arrive(B, s + 1)

        b = Chain(B, lax.rem(s + 1, n), a.u)
        advance("bababbbb", a=(a, "v"), b=(b, "uvu"))
        ucur[...] = b.u
        advance("bb", b=(b, "v"))

    @pl.when(worker)
    def _():
        greet(-1, *range(2, n, 2))
        start_loads()
        v_load.wait()
        vt[B] = vbuf[...].T
        u_load.wait()
        rin[B, 0] = masked(0)
        start_rest()
        begin(ucur[...], 0, enter)
        v_first.wait_recv()

        def first_epoch(s, carry):
            stratum(s, True)
            return carry

        def later_epoch(s, carry):
            stratum(s, False)
            return carry

        lax.fori_loop(0, n - 1, first_epoch, 0)
        lax.fori_loop(n - 1, steps - 1, later_epoch, 0)
        stratum(steps - 1, False, last=True)
        v_last.start()
        vo_ref[...] = vt[B].T
        uo_ref[...] = ucur[...]
        sent = rp.at[pl.ds(1, n - 2)]
        pltpu.make_async_copy(sent, sent, rsend.at[0]).wait()
        pltpu.make_async_copy(uout, uout, usend).wait()
        v_last.wait_send()

    @pl.when(jnp.logical_not(worker))
    def _():
        greet(1, -1)
        start_loads()
        v_load.wait()
        vt[A] = vbuf[...].T
        pl.semaphore_wait(barrier, 1)
        v_first.start()
        u_load.wait()
        u_first.start()
        rp[0] = masked(0)
        r_copy(0, 1).start()
        rp[1] = masked(1)
        r_copy(1, 2).start()
        start_rest()
        wait_all()
        for t in range(2, n):
            rp[t] = masked(t)
        r_copy(0, 1).wait_send()
        pl.semaphore_wait(pace, 1)
        r_copy(2, 1).start()
        r_copy(1, 2).wait_send()
        for t in range(3, n):
            r_copy(t - 1, 1 + (t - 1) % 2).wait_send()
            r_copy(t, 1 + t % 2).start()
        r_copy(n - 1, 1 + (n - 1) % 2).wait_send()
        u_first.wait_send()
        v_first.wait_send()
        u_arrive(steps)
        uo_ref[...] = uin[steps]
        v_last.wait_recv()
        vo_ref[...] = vhome[...].T


def write_out(u_ref, v_ref, uo_ref, vo_ref, sems):
    copies = [pltpu.make_async_copy(v_ref, vo_ref, sems.at[0]), pltpu.make_async_copy(u_ref, uo_ref, sems.at[1])]
    for c in copies:
        c.start()
    for c in copies:
        c.wait()


def solution(mesh):
    n = mesh.shape["shard"]
    row_spec = P(("rep", "shard"), None)

    def local(ratings, observed, user_init, item_init):
        users, rank = user_init.shape
        items = item_init.shape[0]
        scale = (users + items + rank) / math.sqrt(rank)
        eta = 0.5 / scale
        lam = 0.03 * math.sqrt(users * items / rank)
        steps = EPOCHS * n
        vmem = pl.BlockSpec(memory_space=pltpu.VMEM)
        hbm = pl.BlockSpec(memory_space=pltpu.HBM)
        dma = pltpu.SemaphoreType.DMA
        u_last, v_last = pl.pallas_call(
            functools.partial(kernel, n, eta, lam),
            out_shape=(pltpu.VMEM(user_init.shape, F32), pltpu.VMEM(item_init.shape, F32)),
            in_specs=[hbm] * 4,
            out_specs=(vmem, vmem),
            scratch_shapes=[
                pltpu.VMEM((2, users, items), F32),
                pltpu.VMEM((2, users, items), jnp.int32),
                pltpu.VMEM(ratings.shape, F32),
                pltpu.VMEM(observed.shape, jnp.int32),
                pltpu.VMEM((items, rank), F32),
                pltpu.VMEM((n, users, items), F32),
                pltpu.VMEM((2, n, users, items), F32),
                pltpu.VMEM((steps + 1, users, rank), F32),
                pltpu.VMEM((steps, users, rank), F32),
                pltpu.VMEM((users, rank), F32),
                pltpu.VMEM((2, rank, items), F32),
                pltpu.VMEM((rank, items), F32),
                dma((2,)),
                dma,
                dma((2,)),
                dma((3,)),
                dma((2, n)),
                dma,
                dma((n,)),
                dma,
                dma,
                pltpu.SemaphoreType.REGULAR,
            ],
            compiler_params=pltpu.CompilerParams(collective_id=0, has_side_effects=True),
        )(ratings, observed, user_init, item_init)
        return pl.pallas_call(
            write_out,
            out_shape=(jax.ShapeDtypeStruct(user_init.shape, F32), jax.ShapeDtypeStruct(item_init.shape, F32)),
            in_specs=[vmem] * 2,
            out_specs=(hbm, hbm),
            scratch_shapes=[dma((2,))],
            compiler_params=pltpu.CompilerParams(vmem_limit_bytes=2**20),
        )(u_last, v_last)

    return jax.shard_map(local, mesh=mesh, in_specs=(row_spec,) * 4, out_specs=(row_spec, row_spec), check_vma=False)
```

```python
import functools
import math

import jax
import jax.numpy as jnp
from jax import lax
from jax.experimental import pallas as pl
from jax.experimental.pallas import tpu as pltpu
from jax.sharding import PartitionSpec as P

EPOCHS = 2
MESH = pl.DeviceIdType.MESH
F32 = jnp.float32
BF16 = jnp.bfloat16
TILE = 256
A, B = 0, 1


def kernel(
    n, eta, lam, r_ref, m_ref, u_ref, v_ref, uo_ref, vo_ref,
    rbuf, mbuf, rall, mall, vbuf, rp, rin, uin, uout, ucur, vt, vhome,
    rload, mload, allload, uvload, rsend, rrecv, usend, urecv, vsend, vrecv, pace,
):
    items = v_ref.shape[0]
    steps = EPOCHS * n
    me = lax.axis_index("shard")
    worker = lax.rem(me, 2) == 1
    keep = 1.0 - eta * lam

    def dev(offset):
        return {"shard": lax.rem(me + n + offset, n)}

    barrier = pltpu.get_barrier_semaphore()

    def greet(*offsets):
        for d in offsets:
            pl.semaphore_signal(barrier, inc=1, device_id=dev(d), device_id_type=MESH)

    def cols(t):
        return pl.ds(pl.multiple_of(lax.rem(me + t, n) * items, items), items)

    def r_load(t):
        return pltpu.make_async_copy(r_ref.at[:, cols(t)], rbuf.at[t], rload.at[t])

    def m_load(t):
        return pltpu.make_async_copy(m_ref.at[:, cols(t)], mbuf.at[t], mload.at[t])

    u_load = pltpu.make_async_copy(u_ref, ucur, uvload.at[0])
    v_load = pltpu.make_async_copy(v_ref, vbuf, uvload.at[1])

    r_all = pltpu.make_async_copy(r_ref, rall, allload.at[0])
    m_all = pltpu.make_async_copy(m_ref, mall, allload.at[1])

    def start_loads():
        v_load.start()
        u_load.start()
        for t in range(2):
            r_load(t).start()
            m_load(t).start()

    def start_rest():
        r_all.start()
        m_all.start()

    def wait_all():
        r_all.wait()
        m_all.wait()

    def masked(t):
        if isinstance(t, int) and t < 2:
            r_load(t).wait()
            m_load(t).wait()
            return jnp.where(mbuf[t] != 0, rbuf[t], jnp.inf)
        return jnp.where(mall[:, cols(t)] != 0, rall[:, cols(t)], jnp.inf)

    def remote(src, dst, send, recv, device):
        return pltpu.make_async_remote_copy(
            src_ref=src, dst_ref=dst, send_sem=send, recv_sem=recv, device_id=device, device_id_type=MESH
        )

    def r_copy(t, slot=0):
        j = lax.rem(me + t, n)
        chain = lax.rem(j, 2)
        return remote(rp.at[t], rin.at[chain, t], rsend.at[slot], rrecv.at[chain, t], {"shard": j - chain + 1})

    def r_arrive(chain, t):
        remote(rp.at[t], rin.at[chain, t], rsend.at[0], rrecv.at[chain, t], dev(1)).wait_recv()

    def u_copy(s, offset=2):
        return remote(uout.at[s], uin.at[s + 1], usend, urecv.at[lax.rem(s + 1, n)], dev(offset))

    def u_arrive(s):
        remote(ucur, uin.at[s], usend, urecv.at[lax.rem(s, n)], dev(1)).wait_recv()

    u_first = remote(ucur, uin.at[0], usend, urecv.at[0], dev(1))
    v_first = remote(vt.at[A], vt.at[A], vsend, vrecv, dev(1))
    v_last = remote(vt.at[A], vhome, vsend, vrecv, dev(-1))

    def tile(k):
        return pl.ds(k * TILE, TILE)

    class Chain:
        def __init__(self, chain, t, u):
            self.chain, self.t, self.u = chain, t, u

        def predict(self):
            ub = self.u.astype(BF16)
            pred = jnp.dot(ub, vt[self.chain].astype(BF16), preferred_element_type=F32)
            rat = rin[self.chain, self.t]
            err = jnp.where(rat < jnp.inf, pred - rat, 0.0).astype(BF16)
            self.err = [err[:, k * TILE:(k + 1) * TILE] for k in range(items // TILE)]

        def users(self):
            new = keep * self.u
            for k in range(items // TILE):
                vb = vt[self.chain, :, tile(k)].astype(BF16)
                grad = lax.dot_general(self.err[k], vb, (((1,), (1,)), ((), ())), preferred_element_type=F32)
                new = new - eta * grad
            self.u = new

        def items(self):
            ut = self.u.T.astype(BF16)
            for k in range(items // TILE):
                grad = jnp.dot(ut, self.err[k], preferred_element_type=F32)
                vt[self.chain, :, tile(k)] = keep * vt[self.chain, :, tile(k)] - eta * grad

    def advance(order, **work):
        queue = {}
        for name, (chain, kinds) in work.items():
            queue[name] = []
            for kind in kinds:
                queue[name] += [chain.predict, chain.users if kind == "u" else chain.items]
        for name in order:
            queue[name].pop(0)()
        assert not any(queue.values())

    ahead = [[2, n - 2], [3], list(range(4, n - 2))]

    def send_ahead(s):
        @pl.when(s <= len(ahead))
        def _():
            @pl.when(s == 0)
            def _():
                wait_all()

            for k, blocks in enumerate(ahead):
                @pl.when(s == k)
                def _():
                    for t in blocks:
                        rp[t] = masked(t)
                        r_copy(t).start()

            @pl.when(s == len(ahead))
            def _():
                rin[A, n - 1] = masked(n - 1)

    def enter():
        rp[1] = masked(1)
        pl.semaphore_wait(barrier, n // 2 + 1)
        r_copy(1).start()
        pl.semaphore_signal(pace, inc=1, device_id=dev(-1), device_id_type=MESH)

    def begin(u, t, enter):
        b = Chain(B, t, u)
        advance("bbbb", b=(b, "uv"))
        enter()
        advance("bb", b=(b, "u"))
        ucur[...] = b.u
        advance("bb", b=(b, "v"))

    def stratum(s, first, last=False):
        t = s if first else lax.rem(s, n)
        u_arrive(s)
        if first:
            r_arrive(A, s)

        a = Chain(A, t, uin[s])
        b = Chain(B, t, ucur[...])
        advance("abababababab", a=(a, "uvu"), b=(b, "uvu"))
        uout[s] = b.u
        u_copy(s, 1 if last else 2).start()
        if first:
            send_ahead(s)
        advance("aaaababaaa", a=(a, "vuvu"), b=(b, "v"))
        if last:
            advance("aa", a=(a, "v"))
            ucur[...] = a.u
            return
        if first:
            r_arrive(B, s + 1)

        b = Chain(B, lax.rem(s + 1, n), a.u)
        advance("bababbbb", a=(a, "v"), b=(b, "uvu"))
        ucur[...] = b.u
        advance("bb", b=(b, "v"))

    @pl.when(worker)
    def _():
        greet(-1, *range(2, n, 2))
        start_loads()
        v_load.wait()
        vt[B] = vbuf[...].T
        u_load.wait()
        rin[B, 0] = masked(0)
        start_rest()
        begin(ucur[...], 0, enter)
        v_first.wait_recv()

        def first_epoch(s, carry):
            stratum(s, True)
            return carry

        def later_epoch(s, carry):
            stratum(s, False)
            return carry

        lax.fori_loop(0, n - 1, first_epoch, 0)
        lax.fori_loop(n - 1, steps - 1, later_epoch, 0)
        stratum(steps - 1, False, last=True)
        v_last.start()
        vo_ref[...] = vt[B].T
        uo_ref[...] = ucur[...]
        sent = rp.at[pl.ds(1, n - 2)]
        pltpu.make_async_copy(sent, sent, rsend.at[0]).wait()
        pltpu.make_async_copy(uout, uout, usend).wait()
        v_last.wait_send()

    @pl.when(jnp.logical_not(worker))
    def _():
        greet(1, -1)
        start_loads()
        v_load.wait()
        vt[A] = vbuf[...].T
        pl.semaphore_wait(barrier, 1)
        v_first.start()
        u_load.wait()
        u_first.start()
        rp[0] = masked(0)
        r_copy(0, 1).start()
        rp[1] = masked(1)
        r_copy(1, 2).start()
        start_rest()
        wait_all()
        for t in range(2, n):
            rp[t] = masked(t)
        r_copy(0, 1).wait_send()
        pl.semaphore_wait(pace, 1)
        r_copy(2, 1).start()
        r_copy(1, 2).wait_send()
        for t in range(3, n):
            r_copy(t - 1, 1 + (t - 1) % 2).wait_send()
            r_copy(t, 1 + t % 2).start()
        r_copy(n - 1, 1 + (n - 1) % 2).wait_send()
        u_first.wait_send()
        v_first.wait_send()
        u_arrive(steps)
        uo_ref[...] = uin[steps]
        v_last.wait_recv()
        vo_ref[...] = vhome[...].T


def write_out(u_ref, v_ref, uo_ref, vo_ref, sems):
    copies = [pltpu.make_async_copy(v_ref, vo_ref, sems.at[0]), pltpu.make_async_copy(u_ref, uo_ref, sems.at[1])]
    for c in copies:
        c.start()
    for c in copies:
        c.wait()


def solution(mesh):
    n = mesh.shape["shard"]
    row_spec = P(("rep", "shard"), None)

    def local(ratings, observed, user_init, item_init):
        users, rank = user_init.shape
        items = item_init.shape[0]
        scale = (users + items + rank) / math.sqrt(rank)
        eta = 0.5 / scale
        lam = 0.03 * math.sqrt(users * items / rank)
        steps = EPOCHS * n
        vmem = pl.BlockSpec(memory_space=pltpu.VMEM)
        hbm = pl.BlockSpec(memory_space=pltpu.HBM)
        dma = pltpu.SemaphoreType.DMA
        u_last, v_last = pl.pallas_call(
            functools.partial(kernel, n, eta, lam),
            out_shape=(pltpu.VMEM(user_init.shape, F32), pltpu.VMEM(item_init.shape, F32)),
            in_specs=[hbm] * 4,
            out_specs=(vmem, vmem),
            scratch_shapes=[
                pltpu.VMEM((2, users, items), F32),
                pltpu.VMEM((2, users, items), jnp.int32),
                pltpu.VMEM(ratings.shape, F32),
                pltpu.VMEM(observed.shape, jnp.int32),
                pltpu.VMEM((items, rank), F32),
                pltpu.VMEM((n, users, items), F32),
                pltpu.VMEM((2, n, users, items), F32),
                pltpu.VMEM((steps + 1, users, rank), F32),
                pltpu.VMEM((steps, users, rank), F32),
                pltpu.VMEM((users, rank), F32),
                pltpu.VMEM((2, rank, items), F32),
                pltpu.VMEM((rank, items), F32),
                dma((2,)),
                dma((2,)),
                dma((2,)),
                dma((2,)),
                dma((3,)),
                dma((2, n)),
                dma,
                dma((n,)),
                dma,
                dma,
                pltpu.SemaphoreType.REGULAR,
            ],
            compiler_params=pltpu.CompilerParams(collective_id=0, has_side_effects=True),
        )(ratings, observed, user_init, item_init)
        return pl.pallas_call(
            write_out,
            out_shape=(jax.ShapeDtypeStruct(user_init.shape, F32), jax.ShapeDtypeStruct(item_init.shape, F32)),
            in_specs=[vmem] * 2,
            out_specs=(hbm, hbm),
            scratch_shapes=[dma((2,))],
            compiler_params=pltpu.CompilerParams(vmem_limit_bytes=2**20),
        )(u_last, v_last)

    return jax.shard_map(local, mesh=mesh, in_specs=(row_spec,) * 4, out_specs=(row_spec, row_spec), check_vma=False)
```
